32 devices in a mesh: group: 2 (over x), lat: 16 (over z, y, core).
Axes of the slice: x: 2, y: 2, z: 4, core: 2. Of those that a mesh axis runs over, the one named last changes fastest.
Arguments:
- grid_values: bfloat16 [224, 1440, 256], P(('group', 'lat')), parts along dimension 0, may hold values from -630 to 630
- lat_counts: int32 [16], replicated, may hold values from 1 to 7, 96 in all
- owner_wavenumber: int32 [384], replicated, may hold values from 0 to 383, each once
- legendre: bfloat16 [384, 96, 384], P('lat'), may hold values from -0.625 to 0.625
- quad_weight: float32 [96], replicated, may hold values from 0.3 to 3
- spectral_gain: float32 [384, 256], replicated, may hold values from 0.3 to 3
- channel_mix: bfloat16 [256, 256], replicated, may hold values from -0.375 to 0.375
Outputs:
- grid_output: bfloat16 [224, 1440, 256], P(('group', 'lat')), parts along dimension 0
The draws below stay inside these ranges and needn't reach their ends.
There are 2 independent parts, one for each index of `group`. The reference program is written for one: setup_inputs(seed, part) draws one part's arguments, and reference() takes and returns one part's arrays. A program takes and returns all parts, laid end to end along the dimension named above; an argument that names none is the same for every part. Nothing has to cross between parts.
Inputs may be any that keep to these rules, and one draw needn't show every extreme that they name: `lat_counts`: some device has all 7 slots live. `owner_wavenumber`: each wavenumber appears once; device i of lat owns wavenumber slots i * 24 to (i + 1) * 24 - 1.
All inputs are finite; a program needn't handle non-finite values.
Results may differ from the reference program's by a relative error of at most 0.0095.
Values may be sent and summed in bfloat16 or wider, within the bound.
A program may use at most 64 MiB of HBM per device.

```python
import math
import jax
import jax.numpy as jnp
import numpy as np
from jax import lax

LONGITUDES = 1440
CHANNELS = 256
WAVES = 384
DEGREES = 384
LAT_SLOTS = 7
SLOTS_ALL = 112
LIVE_LATS = 96
N_LAT = 16


def draw_grid_values(key, part):
    key_rows = jax.random.fold_in(key, 11)
    key_scale = jax.random.fold_in(key, 12)
    key_mean = jax.random.fold_in(key, 13)
    key_noise = jax.random.fold_in(key, 14)
    position = jnp.arange(SLOTS_ALL, dtype=jnp.float32) / SLOTS_ALL
    jitter = jax.random.uniform(key_rows, (SLOTS_ALL,), minval=-0.1, maxval=0.1)
    row_scale = jnp.exp(jnp.log(10.0) * jnp.clip(position + jitter, 0.0, 1.0))
    chan_scale = jnp.exp(jax.random.uniform(key_scale, (CHANNELS,), minval=0.0, maxval=jnp.log(10.0)))
    chan_mean = jax.random.uniform(key_mean, (CHANNELS,), minval=-1.0, maxval=1.0)
    noise = jnp.clip(jax.random.normal(key_noise, (SLOTS_ALL, LONGITUDES, CHANNELS)), -6.0, 6.0)
    values = chan_mean[None, None, :] * chan_scale[None, None, :] + row_scale[:, None, None] * chan_scale[None, None, :] * noise
    return values.astype(jnp.float32).astype(jnp.bfloat16)


def block_levels(rng, shape, cuts, low, top_value):
    loudness, own = 1.0, jax.random.fold_in(rng, 6)
    for dim, blocks in cuts:
        heights = jnp.exp(jax.random.uniform(jax.random.fold_in(own, dim), (blocks,), jnp.float32, low / len(cuts), top_value / len(cuts)))
        loudness = loudness * jnp.repeat(heights, shape[dim] // blocks).reshape([-1 if axis == dim else 1 for axis in range(len(shape))])
    return loudness


def length_profile(number_of, total, reach, lean):
    weights = [(1 << 20) // math.isqrt(rank ** lean) + 1 for rank in range(2, number_of + 1)]
    spare, given = total - reach - (number_of - 1), [1] * (number_of - 1)
    while spare > 0:
        movable = [i for i in range(number_of - 1) if given[i] < reach]
        mass, budget = sum([weights[i] for i in movable]), spare
        for i in movable:
            extra = min(reach - given[i], max(1, budget * weights[i] // mass), spare)
            given[i] = given[i] + extra
            spare = spare - extra
    return np.array([reach] + given)


def ragged(key, amount, total, bound, slope):
    if amount == 2:
        one = jax.random.randint(key, (), max(1, total - bound), min(bound, total - 1) + 1)
        return jnp.stack([one, total - one])
    lengths = jnp.asarray(length_profile(amount, total, bound, slope), jnp.int32)
    pairs = (amount - 1) // 2
    giver, sink = lengths[1:1 + 2 * pairs:2], lengths[2:2 + 2 * pairs:2]
    room = jnp.minimum(giver - 1, bound - sink)
    shifted = jax.random.randint(jax.random.fold_in(key, 1), (pairs,), 0, 1 << 20) % (room + 1)
    lengths = lengths.at[1:1 + 2 * pairs:2].set(giver - shifted).at[2:2 + 2 * pairs:2].set(sink + shifted)
    return lengths[jax.random.permutation(jax.random.fold_in(key, 2), amount)]


def scatter_about(rng, extent, spread, limit, split=(), held_as=jnp.bfloat16):
    level = block_levels(rng, extent, split, -0.22, 0.18) if split else 1.0
    values = jax.random.normal(rng, extent, jnp.float32) * spread * level
    return jnp.minimum(jnp.maximum(values, -limit), limit).astype(held_as)


def setup_inputs(seed: int = 0, part: int = 0) -> dict:
    splits = jax.random.split(jax.random.key(seed), 8)
    own_keys = jax.random.split(jax.random.fold_in(splits[7], part), 8)
    return {
        "grid_values": draw_grid_values(jax.random.fold_in(jax.random.fold_in(splits[7], part), 71), part),
        "lat_counts": ragged(splits[1], N_LAT, LIVE_LATS, LAT_SLOTS, 2).astype(jnp.int32),
        "owner_wavenumber": jax.random.permutation(splits[2], WAVES).astype(jnp.int32),
        "legendre": scatter_about(splits[3], (WAVES, LIVE_LATS, DEGREES), LIVE_LATS ** -0.5, 0.625, ((0, 16),)),
        "quad_weight": jnp.clip(jnp.exp(jax.random.uniform(splits[4], (LIVE_LATS,), jnp.float32, math.log(0.3), math.log(3.0))), 0.3, 3.0),
        "spectral_gain": jnp.clip(jnp.exp(jax.random.uniform(splits[5], (DEGREES, CHANNELS), jnp.float32, math.log(0.3), math.log(3.0))), 0.3, 3.0),
        "channel_mix": scatter_about(splits[6], (CHANNELS, CHANNELS), CHANNELS ** -0.5, 0.375),
    }


def live_slots(lat_counts, slot_count, live_total):
    devices = lat_counts.shape[0]
    starts = jnp.cumsum(lat_counts) - lat_counts
    device_ids = jnp.arange(devices, dtype=jnp.int32)
    slot_ids = jnp.arange(devices * slot_count, dtype=jnp.int32)
    holder = slot_ids // slot_count
    within = slot_ids - holder * slot_count
    holder_hot = holder[:, None] == device_ids[None, :]
    holder_count = lax.optimization_barrier(jnp.sum(jnp.where(holder_hot, lat_counts[None, :], 0), axis=1))
    holder_start = lax.optimization_barrier(jnp.sum(jnp.where(holder_hot, starts[None, :], 0), axis=1))
    slot_valid = within < holder_count
    slot_live = jnp.where(slot_valid, holder_start + within, 0).astype(jnp.int32)
    live_ids = jnp.arange(live_total, dtype=jnp.int32)
    reached = (starts[None, :] <= live_ids[:, None]).astype(jnp.int32)
    source = lax.optimization_barrier(jnp.sum(reached, axis=1)) - 1
    source_hot = source[:, None] == device_ids[None, :]
    source_start = lax.optimization_barrier(jnp.sum(jnp.where(source_hot, starts[None, :], 0), axis=1))
    live_slot = (source * slot_count + live_ids - source_start).astype(jnp.int32)
    return (slot_valid, slot_live, live_slot)

def wave_angles(wave_list, longitudes):
    points = jnp.arange(longitudes, dtype=jnp.int32)
    phase = wave_list[:, None] * points[None, :] % longitudes
    return phase.astype(jnp.float32) * (2.0 * math.pi / longitudes)

def forward_table(wave_list, longitudes):
    angle = wave_angles(wave_list, longitudes)
    factor = 1.0 / math.sqrt(longitudes)
    return jnp.stack([jnp.cos(angle) * factor, -jnp.sin(angle) * factor], axis=1).astype(jnp.bfloat16)

def inverse_table(wave_list, longitudes):
    angle = wave_angles(wave_list, longitudes)
    factor = 1.0 / math.sqrt(longitudes)
    doubled = jnp.where(wave_list > 0, 2.0, 1.0).astype(jnp.float32)[:, None] * factor
    return jnp.stack([jnp.cos(angle) * doubled, -jnp.sin(angle) * doubled], axis=1).astype(jnp.bfloat16)

def reference(grid_values, lat_counts, owner_wavenumber, legendre, quad_weight, spectral_gain, channel_mix):
    slot_valid, slot_live, live_slot = live_slots(lat_counts, LAT_SLOTS, LIVE_LATS)
    row_weight = slot_valid.astype(jnp.float32)[:, None, None]
    widened = grid_values.astype(jnp.float32) * row_weight
    points = LIVE_LATS * LONGITUDES
    channel_mean = lax.optimization_barrier(jnp.sum(widened, axis=(0, 1))) / points
    variance = lax.optimization_barrier(jnp.sum(widened * widened, axis=(0, 1))) / points - channel_mean * channel_mean
    normed = ((grid_values.astype(jnp.float32) - channel_mean) * lax.rsqrt(variance + 1e-05) * row_weight).astype(jnp.bfloat16)
    forward = forward_table(owner_wavenumber, LONGITUDES)
    spectra = jnp.einsum('skc,rtk->srtc', normed.astype(jnp.float32), forward.astype(jnp.float32)).astype(jnp.bfloat16)
    gathered = jnp.take(spectra, live_slot, axis=0)
    weighted = (gathered.astype(jnp.float32) * quad_weight[:, None, None, None]).astype(jnp.bfloat16)
    coefficient = jnp.einsum('rgl,grtc->rltc', legendre.astype(jnp.float32), weighted.astype(jnp.float32))
    degree_mask = (jnp.arange(DEGREES, dtype=jnp.int32)[None, :] >= owner_wavenumber[:, None]).astype(jnp.float32)
    filtered = (coefficient * degree_mask[:, :, None, None] * spectral_gain[None, :, None, :]).astype(jnp.bfloat16)
    mixed = jnp.dot(filtered.reshape(-1, CHANNELS), channel_mix, preferred_element_type=jnp.float32)
    mixed = mixed.astype(jnp.bfloat16).reshape(WAVES, DEGREES, 2, CHANNELS)
    synthesis = jnp.einsum('rgl,rltc->grtc', legendre.astype(jnp.float32), mixed.astype(jnp.float32)).astype(jnp.bfloat16)
    outgoing = jnp.where(slot_valid[:, None, None, None], jnp.take(synthesis, slot_live, axis=0), jnp.zeros((), jnp.bfloat16))
    inverse = inverse_table(owner_wavenumber, LONGITUDES)
    result = jnp.einsum('srtc,rtk->skc', outgoing.astype(jnp.float32), inverse.astype(jnp.float32))
    return result.astype(jnp.bfloat16)
```

```python
import functools
import math

import jax
import jax.numpy as jnp
import numpy as np
from jax import lax
from jax.experimental import pallas as pl
from jax.experimental.pallas import tpu as pltpu
from jax.sharding import PartitionSpec as P

BLOCK = 8
F32 = jnp.float32
BF16 = jnp.bfloat16


def trig_table(waves, longitudes):
    phase = np.arange(waves)[:, None] * np.arange(longitudes)[None, :] % longitudes
    angle = phase * (2.0 * math.pi / longitudes)
    factor = 1.0 / math.sqrt(longitudes)
    table = np.concatenate([np.cos(angle) * factor, -np.sin(angle) * factor], axis=0)
    return table.astype(BF16)


def greet_all(axis, count, me):
    barrier = pltpu.get_barrier_semaphore()

    def signal(i, carry):
        other = lax.rem(me + i, count)
        pl.semaphore_signal(
            barrier, inc=1, device_id={axis: other}, device_id_type=pl.DeviceIdType.MESH
        )
        return carry

    lax.fori_loop(1, count, signal, 0)
    return barrier


def spectral_kernel(
    axis, n, points, share, counts, owner, row_sum, x, base_far, legendre_far, quad, gain_far,
    mix, last, back_table, partial,
    sums, rows, hot, table, front, spec, recv, gathered, pick, quad_slot, outgoing, result,
    early, base, legendre, gain,
    load, fetch, mom_send, mom_recv, send, arrive, own, back_send, back_arrive, back_own,
):
    me = lax.axis_index(axis)
    slots, longitudes, channels = x.shape
    everything = n * slots
    live_total, degrees = legendre.shape[1], legendre.shape[2]
    halves = channels // 128
    blocks = spec.shape[0]
    lines = n * 2 * BLOCK
    waves = base.shape[0] // 2

    def load_slot(s):
        return pltpu.make_async_copy(x.at[s], partial.at[s], load.at[s])

    def start_load(s, carry):
        load_slot(s).start()
        return carry

    base_copy = pltpu.make_async_copy(base_far, base, fetch.at[0])
    legendre_copy = pltpu.make_async_copy(legendre_far, legendre, fetch.at[1])
    gain_copy = pltpu.make_async_copy(gain_far, gain, fetch.at[2])
    base_copy.start()
    lax.fori_loop(0, slots, start_load, 0)
    legendre_copy.start()
    gain_copy.start()
    barrier = greet_all(axis, n, me)

    row_of = lax.broadcasted_iota(jnp.int32, (BLOCK, waves), 0)
    lane_of = lax.broadcasted_iota(jnp.int32, (BLOCK, waves), 1)

    def choose_rows(o, carry):
        for b in range(blocks):
            count = min(BLOCK, share - b * BLOCK)
            held = jnp.full((BLOCK, waves), -1, jnp.int32)
            for r in range(count):
                held = jnp.where(row_of == r, owner[o * share + b * BLOCK + r], held)
            begin = pl.multiple_of((b * n + o) * BLOCK, BLOCK)
            hot[pl.ds(begin, BLOCK), :] = jnp.where(lane_of == held, 1.0, 0.0).astype(F32)
        return carry

    lax.fori_loop(0, n, choose_rows, 0)
    live = counts[me]
    group = math.gcd(longitudes, 32)

    def build_table(b):
        chosen = hot[b * n * BLOCK : (b + 1) * n * BLOCK, :].astype(BF16)
        both = [
            jnp.dot(chosen, base[t * waves : (t + 1) * waves], preferred_element_type=F32)
            for t in range(2)
        ]
        both = [part.reshape(n, 1, BLOCK, longitudes) for part in both]
        both = jnp.concatenate(both, axis=1).reshape(lines, longitudes)
        table[b * lines : (b + 1) * lines] = both.astype(BF16)

    def transform(b, s):
        out = jnp.dot(table[b * lines : (b + 1) * lines], partial[s], preferred_element_type=F32)
        spec[b, :, s] = out.astype(BF16).reshape(n, 2 * BLOCK, channels)

    def add_slot(s, second):
        wide = partial[s].astype(F32).reshape(-1, group, channels)
        weight = jnp.where(s < live, 1.0, 0.0).astype(F32)
        first = weight * jnp.sum(wide, axis=0)
        sums[me, pl.ds(s, 1), :] = jnp.sum(first, axis=0, keepdims=True)
        return second + weight * jnp.sum(wide * wide, axis=0)

    def slice_copy(b, i, first, size):
        other = lax.rem(me + i, n)
        return pltpu.make_async_remote_copy(
            src_ref=spec.at[b, other, pl.ds(first, size)],
            dst_ref=recv.at[b, me, pl.ds(first, size)],
            send_sem=send.at[b, i], recv_sem=arrive.at[b, i],
            device_id={axis: other}, device_id_type=pl.DeviceIdType.MESH,
        )

    def block_copy(b, i):
        return slice_copy(b, i, 0, slots)

    def send_slices(b, first, size):
        def start_slices(i, carry):
            slice_copy(b, i, first, size).start()
            return carry

        lax.fori_loop(1, n, start_slices, 0)

    def moment_copy(i):
        other = lax.rem(me + i, n)
        return pltpu.make_async_remote_copy(
            src_ref=sums.at[me], dst_ref=sums.at[me],
            send_sem=mom_send.at[i], recv_sem=mom_recv.at[i],
            device_id={axis: other}, device_id_type=pl.DeviceIdType.MESH,
        )

    def start_moment(i, carry):
        moment_copy(i).start()
        return carry

    def wait_moment(i, carry):
        moment_copy(i).wait()
        return carry

    def own_copy(b):
        return pltpu.make_async_copy(spec.at[b, me], recv.at[b, me], own.at[b])

    base_copy.wait()
    build_table(0)
    load_slot(0).wait()
    transform(0, 0)
    pl.semaphore_wait(barrier, n - 1)
    send_slices(0, 0, 1)

    def first_slot(s, carry):
        load_slot(s).wait()
        transform(0, s)
        return carry

    cuts = [1, 1 + (slots - 1) // 3, slots]
    for first, end in zip(cuts[:-1], cuts[1:]):
        if end > first:
            lax.fori_loop(first, end, first_slot, 0)
            send_slices(0, first, end - first)
    own_copy(0).start()
    second = lax.fori_loop(0, slots, add_slot, jnp.zeros((group, channels), F32))
    sums[me, slots : slots + 1, :] = jnp.sum(second, axis=0, keepdims=True)
    lax.fori_loop(1, n, start_moment, 0)
    for b in range(1, blocks):
        build_table(b)

        def slot_step(s, carry):
            transform(b, s)
            return carry

        lax.fori_loop(0, slots, slot_step, 0)
        send_slices(b, 0, slots)
        own_copy(b).start()

    late = (blocks - 1) * lines
    back_table[...] = table[late:].T
    if blocks > 1:
        front[...] = table[:late].T
    legendre_copy.wait()
    gain_copy.wait()
    row = lax.broadcasted_iota(jnp.int32, (everything, live_total), 0)
    lane = lax.broadcasted_iota(jnp.int32, (everything, live_total), 1)
    pick[...] = jnp.zeros_like(pick)

    def mark(i, begin):
        within = row - i * slots
        hit = (within >= 0) & (within < counts[i]) & (lane == begin + within)
        pick[...] += jnp.where(hit, 1.0, 0.0).astype(F32)
        return begin + counts[i]

    lax.fori_loop(0, n, mark, jnp.int32(0))
    quad_slot[...] = jnp.broadcast_to(
        jnp.sum(pick[...] * quad[...], axis=1, keepdims=True), quad_slot.shape
    )
    degree = lax.broadcasted_iota(jnp.int32, (degrees, channels), 0)
    lax.fori_loop(1, n, wait_moment, 0)
    totals = jnp.sum(sums[...], axis=0)
    mean = jnp.sum(totals[0:slots], axis=0, keepdims=True) / points
    variance = totals[slots : slots + 1] / points - mean * mean
    gain[...] = gain[...] * lax.rsqrt(variance + 1e-05)
    for i in range(n):
        rows[i * slots : (i + 1) * slots, :] = sums[i, 0:slots, :]
    level = float(np.asarray(1.0 / math.sqrt(longitudes)).astype(BF16))

    def landing(b):
        return early.at[b, me] if b < blocks - 1 else last.at[me]

    def return_copy(b, i):
        other = lax.rem(me + i, n)
        return pltpu.make_async_remote_copy(
            src_ref=outgoing.at[b, other], dst_ref=landing(b),
            send_sem=back_send.at[b, i], recv_sem=back_arrive.at[b, i],
            device_id={axis: other}, device_id_type=pl.DeviceIdType.MESH,
        )

    for b in range(blocks):
        count = min(BLOCK, share - b * BLOCK)
        if count < BLOCK:
            result[...] = jnp.zeros_like(result)

        def wait_block(i, carry):
            block_copy(b, i).wait()
            return carry

        lax.fori_loop(1, n, wait_block, 0)
        own_copy(b).wait()

        def widen(i, carry):
            for s in range(slots):
                wide = recv[b, i, s].astype(F32)
                begin = pl.multiple_of((i * slots + s) * 2 * BLOCK, 8)
                for h in range(halves):
                    gathered[h, pl.ds(begin, 2 * BLOCK), :] = wide[:, h * 128 : (h + 1) * 128]
            return carry

        lax.fori_loop(0, n, widen, 0)

        def wave_step(r, carry):
            wave = owner[me * share + b * BLOCK + r]
            expanded = jnp.dot(
                pick[...].astype(BF16), legendre[b * BLOCK + r], preferred_element_type=F32
            ).astype(BF16)
            pieces = []
            for t in range(2):
                for h in range(halves):
                    lanes = slice(h * 128, (h + 1) * 128)
                    piece = gathered[h, pl.ds(t * BLOCK + r, everything, stride=2 * BLOCK), :]
                    if t == 0:
                        piece = jnp.where(wave == 0, rows[:, lanes] * level, piece)
                    piece = piece - mean[:, lanes] * row_sum[t * waves + wave]
                    pieces.append((piece * quad_slot[...]).astype(BF16))
            weighted = jnp.concatenate(pieces, axis=1)
            coefficient = lax.dot_general(
                expanded, weighted, (((0,), (0,)), ((), ())), preferred_element_type=F32
            )
            kept = degree >= wave
            factor = jnp.where(wave > 0, 2.0, 1.0).astype(F32)
            mixed = []
            for t in range(2):
                part = coefficient[:, t * channels : (t + 1) * channels] * gain[...]
                part = jnp.where(kept, part, 0.0).astype(BF16)
                mixed.append(jnp.dot(part, mix[...], preferred_element_type=F32).astype(BF16))
            synthesis = jnp.dot(
                expanded, jnp.concatenate(mixed, axis=1), preferred_element_type=F32
            ) * factor
            for t in range(2):
                for h in range(halves):
                    begin = t * channels + h * 128
                    result[h, pl.ds(t * BLOCK + r, everything, stride=2 * BLOCK), :] = synthesis[
                        :, begin : begin + 128
                    ]
            return carry

        lax.fori_loop(0, count, wave_step, 0)

        def narrow(i, carry):
            for s in range(slots):
                begin = pl.multiple_of((i * slots + s) * 2 * BLOCK, 8)
                outgoing[b, i, s] = jnp.concatenate(
                    [result[h, pl.ds(begin, 2 * BLOCK), :] for h in range(halves)], axis=1
                ).astype(BF16)
            return carry

        lax.fori_loop(0, n, narrow, 0)

        def start_return(i, carry):
            return_copy(b, i).start()
            return carry

        lax.fori_loop(1, n, start_return, 0)
        pltpu.make_async_copy(outgoing.at[b, me], landing(b), back_own.at[b]).start()

    def settle(b):
        def wait_return(i, carry):
            return_copy(b, i).wait()
            return carry

        lax.fori_loop(1, n, wait_return, 0)
        pltpu.make_async_copy(outgoing.at[b, me], landing(b), back_own.at[b]).wait()

    for b in range(blocks - 1):
        settle(b)

    def partial_slot(s, carry):
        if blocks > 1:
            block = early[:, :, s].reshape(late, channels)
            partial[s] = jnp.dot(front[...], block, preferred_element_type=F32).astype(BF16)
        else:
            partial[s] = jnp.zeros(partial.shape[1:], BF16)
        return carry

    lax.fori_loop(0, slots, partial_slot, 0)
    settle(blocks - 1)


def inverse_kernel(last, table, partial, out, held, store):
    slots = partial.shape[0]

    def store_slot(s):
        return pltpu.make_async_copy(held.at[s], out.at[s], store.at[s])

    def finish_slot(s, carry):
        block = last[:, s].reshape(table.shape[1], last.shape[-1])
        total = jnp.dot(table[...], block, preferred_element_type=F32)
        held[s] = (partial[s].astype(F32) + total).astype(BF16)
        store_slot(s).start()
        return carry

    def wait_store(s, carry):
        store_slot(s).wait()
        return carry

    lax.fori_loop(0, slots, finish_slot, 0)
    lax.fori_loop(0, slots, wait_store, 0)


def body(
    n, grid_values, lat_counts, owner_wavenumber, legendre, quad_weight, spectral_gain, channel_mix
):
    slots, longitudes, channels = grid_values.shape
    waves = owner_wavenumber.shape[0]
    share, live_total, degrees = legendre.shape
    blocks = -(-share // BLOCK)
    padded = blocks * BLOCK
    everything = n * slots
    trig = trig_table(waves, longitudes)
    base = jnp.asarray(trig)
    row_sum = jnp.asarray(trig.astype(np.float64).sum(axis=1).astype(np.float32))

    vmem = pl.BlockSpec(memory_space=pltpu.VMEM)
    smem = pl.BlockSpec(memory_space=pltpu.SMEM)
    anywhere = pl.BlockSpec(memory_space=pl.ANY)
    limit = 48 * 1024 * 1024
    packet = (blocks, n, slots, 2 * BLOCK, channels)
    copies = pltpu.SemaphoreType.DMA
    lines = n * 2 * BLOCK
    last, back_table, partial = pl.pallas_call(
        functools.partial(spectral_kernel, "lat", n, live_total * longitudes, share),
        out_shape=(
            pltpu.VMEM(packet[1:], BF16),
            pltpu.VMEM((longitudes, lines), BF16),
            pltpu.VMEM((slots, longitudes, channels), BF16),
        ),
        in_specs=[smem, smem, smem, anywhere, anywhere, anywhere, vmem, anywhere, vmem],
        out_specs=(vmem, vmem, vmem),
        scratch_shapes=[
            pltpu.VMEM((n, slots + 1, channels), F32),
            pltpu.VMEM((everything, channels), F32),
            pltpu.VMEM((n * padded, waves), F32),
            pltpu.VMEM((blocks * lines, longitudes), BF16),
            pltpu.VMEM((longitudes, max(blocks - 1, 1) * lines), BF16),
            pltpu.VMEM(packet, BF16),
            pltpu.VMEM(packet, BF16),
            pltpu.VMEM((channels // 128, everything * 2 * BLOCK, 128), F32),
            pltpu.VMEM((everything, live_total), F32),
            pltpu.VMEM((everything, 128), F32),
            pltpu.VMEM(packet, BF16),
            pltpu.VMEM((channels // 128, everything * 2 * BLOCK, 128), F32),
            pltpu.VMEM((max(blocks - 1, 1),) + packet[1:], BF16),
            pltpu.VMEM(base.shape, BF16),
            pltpu.VMEM(legendre.shape, BF16),
            pltpu.VMEM(spectral_gain.shape, F32),
            copies((slots,)), copies((3,)),
            copies((n,)), copies((n,)),
            copies((blocks, n)), copies((blocks, n)), copies((blocks,)),
            copies((blocks, n)), copies((blocks, n)), copies((blocks,)),
        ],
        compiler_params=pltpu.CompilerParams(
            collective_id=0, has_side_effects=True, vmem_limit_bytes=limit
        ),
    )(
        lat_counts, owner_wavenumber, row_sum, grid_values, base, legendre,
        quad_weight.reshape(1, live_total), spectral_gain, channel_mix,
    )

    return pl.pallas_call(
        inverse_kernel,
        out_shape=jax.ShapeDtypeStruct((slots, longitudes, channels), BF16),
        in_specs=[vmem, vmem, vmem],
        out_specs=anywhere,
        scratch_shapes=[
            pltpu.VMEM((slots, longitudes, channels), BF16),
            copies((slots,)),
        ],
        compiler_params=pltpu.CompilerParams(vmem_limit_bytes=16 * 1024 * 1024),
    )(*[pltpu.with_memory_space_constraint(v, pltpu.VMEM) for v in (last, back_table, partial)])


def solution(mesh):
    return jax.shard_map(
        functools.partial(body, mesh.shape["lat"]),
        mesh=mesh,
        in_specs=(P(("group", "lat"), None, None), P(), P(), P("lat", None, None), P(), P(), P()),
        out_specs=P(("group", "lat"), None, None),
        check_vma=False,
    )
```

```python
import functools
import math

import jax
import jax.numpy as jnp
import numpy as np
from jax import lax
from jax.experimental import pallas as pl
from jax.experimental.pallas import tpu as pltpu
from jax.sharding import PartitionSpec as P

BLOCK = 8
TAIL = 1
F32 = jnp.float32
BF16 = jnp.bfloat16


def trig_table(waves, longitudes):
    phase = np.arange(waves)[:, None] * np.arange(longitudes)[None, :] % longitudes
    angle = phase * (2.0 * math.pi / longitudes)
    factor = 1.0 / math.sqrt(longitudes)
    table = np.concatenate([np.cos(angle) * factor, -np.sin(angle) * factor], axis=0)
    return table.astype(BF16)


def greet_all(axis, count, me):
    barrier = pltpu.get_barrier_semaphore()

    def signal(i, carry):
        other = lax.rem(me + i, count)
        pl.semaphore_signal(
            barrier, inc=1, device_id={axis: other}, device_id_type=pl.DeviceIdType.MESH
        )
        return carry

    lax.fori_loop(1, count, signal, 0)
    return barrier


def spectral_kernel(
    axis, n, points, share, counts, owner, row_sum, x, base_far, legendre_far, quad, gain_far,
    mix, last, back_table, partial,
    sums, zero, hot, table, front, spec, recv, gathered, pick, quad_slot, outgoing, result,
    early, late, base, legendre, gain,
    load, fetch, mom_send, mom_recv, send, arrive, own, back_send, back_arrive, back_own,
):
    me = lax.axis_index(axis)
    slots, longitudes, channels = x.shape
    everything = n * slots
    live_total, degrees = legendre.shape[1], legendre.shape[2]
    halves = channels // 128
    blocks = spec.shape[0]
    lines = n * 2 * BLOCK
    waves = base.shape[0] // 2
    ready = slots - last.shape[1]

    def load_slot(s):
        return pltpu.make_async_copy(x.at[s], partial.at[s], load.at[s])

    def start_load(s, carry):
        load_slot(s).start()
        return carry

    base_copy = pltpu.make_async_copy(base_far, base, fetch.at[0])
    legendre_copy = pltpu.make_async_copy(legendre_far, legendre, fetch.at[1])
    gain_copy = pltpu.make_async_copy(gain_far, gain, fetch.at[2])
    base_copy.start()
    lax.fori_loop(0, slots, start_load, 0)
    legendre_copy.start()
    gain_copy.start()
    barrier = greet_all(axis, n, me)

    row_of = lax.broadcasted_iota(jnp.int32, (BLOCK, waves), 0)
    lane_of = lax.broadcasted_iota(jnp.int32, (BLOCK, waves), 1)

    def choose_rows(o, carry):
        for b in range(blocks):
            count = min(BLOCK, share - b * BLOCK)
            held = jnp.full((BLOCK, waves), -1, jnp.int32)
            for r in range(count):
                held = jnp.where(row_of == r, owner[o * share + b * BLOCK + r], held)
            begin = pl.multiple_of((b * n + o) * BLOCK, BLOCK)
            hot[pl.ds(begin, BLOCK), :] = jnp.where(lane_of == held, 1.0, 0.0).astype(F32)
        return carry

    lax.fori_loop(0, n, choose_rows, 0)
    zero[...] = jnp.broadcast_to(hot[:, 0:1], zero.shape)
    live = counts[me]
    group = math.gcd(longitudes, 32)

    def build_table(b):
        chosen = hot[b * n * BLOCK : (b + 1) * n * BLOCK, :].astype(BF16)
        both = [
            jnp.dot(chosen, base[t * waves : (t + 1) * waves], preferred_element_type=F32)
            for t in range(2)
        ]
        both = [part.reshape(n, 1, BLOCK, longitudes) for part in both]
        both = jnp.concatenate(both, axis=1).reshape(lines, longitudes)
        table[b * lines : (b + 1) * lines] = both.astype(BF16)

    def transform(b, s):
        out = jnp.dot(table[b * lines : (b + 1) * lines], partial[s], preferred_element_type=F32)
        out = out.reshape(n, 2, BLOCK, channels)
        real, imag = out[:, 0], out[:, 1]
        flag = zero[b * n * BLOCK : (b + 1) * n * BLOCK].reshape(n, BLOCK, channels)
        imag = imag + flag * (real - real.astype(BF16).astype(F32))
        out = jnp.concatenate([real, imag], axis=1)
        spec[b, :, s] = out.astype(BF16)

    def add_slot(s, carry):
        first, second = carry
        wide = partial[s].astype(F32).reshape(-1, group, channels)
        weight = jnp.where(s < live, 1.0, 0.0).astype(F32)
        first = first + weight * jnp.sum(wide, axis=0)
        second = second + weight * jnp.sum(wide * wide, axis=0)
        return first, second

    def slice_copy(b, i, first, size):
        other = lax.rem(me + i, n)
        return pltpu.make_async_remote_copy(
            src_ref=spec.at[b, other, pl.ds(first, size)],
            dst_ref=recv.at[b, me, pl.ds(first, size)],
            send_sem=send.at[b, i], recv_sem=arrive.at[b, i],
            device_id={axis: other}, device_id_type=pl.DeviceIdType.MESH,
        )

    def block_copy(b, i):
        return slice_copy(b, i, 0, slots)

    def send_slices(b, first, size):
        def start_slices(i, carry):
            slice_copy(b, i, first, size).start()
            return carry

        lax.fori_loop(1, n, start_slices, 0)

    def moment_copy(i):
        other = lax.rem(me + i, n)
        return pltpu.make_async_remote_copy(
            src_ref=sums.at[me], dst_ref=sums.at[me],
            send_sem=mom_send.at[i], recv_sem=mom_recv.at[i],
            device_id={axis: other}, device_id_type=pl.DeviceIdType.MESH,
        )

    def start_moment(i, carry):
        moment_copy(i).start()
        return carry

    def wait_moment(i, carry):
        moment_copy(i).wait()
        return carry

    def own_copy(b):
        return pltpu.make_async_copy(spec.at[b, me], recv.at[b, me], own.at[b])

    base_copy.wait()
    build_table(0)
    load_slot(0).wait()
    transform(0, 0)
    pl.semaphore_wait(barrier, n - 1)
    send_slices(0, 0, 1)

    def first_slot(s, carry):
        load_slot(s).wait()
        transform(0, s)
        return carry

    cuts = [1, 1 + (slots - 1) // 3, slots]
    for first, end in zip(cuts[:-1], cuts[1:]):
        if end > first:
            lax.fori_loop(first, end, first_slot, 0)
            send_slices(0, first, end - first)
    own_copy(0).start()
    nothing = jnp.zeros((group, channels), F32)
    first, second = lax.fori_loop(0, slots, add_slot, (nothing, nothing))
    sums[me, 0:1, :] = jnp.sum(first, axis=0, keepdims=True)
    sums[me, 1:2, :] = jnp.sum(second, axis=0, keepdims=True)
    lax.fori_loop(1, n, start_moment, 0)
    for b in range(1, blocks):
        build_table(b)

        def slot_step(s, carry):
            transform(b, s)
            return carry

        lax.fori_loop(0, slots, slot_step, 0)
        send_slices(b, 0, slots)
        own_copy(b).start()

    split = (blocks - 1) * lines
    back_table[...] = table[split:].T
    if blocks > 1:
        front[...] = table[:split].T
    legendre_copy.wait()
    gain_copy.wait()
    row = lax.broadcasted_iota(jnp.int32, (everything, live_total), 0)
    lane = lax.broadcasted_iota(jnp.int32, (everything, live_total), 1)
    pick[...] = jnp.zeros_like(pick)

    def mark(i, begin):
        within = row - i * slots
        hit = (within >= 0) & (within < counts[i]) & (lane == begin + within)
        pick[...] += jnp.where(hit, 1.0, 0.0).astype(F32)
        return begin + counts[i]

    lax.fori_loop(0, n, mark, jnp.int32(0))
    quad_slot[...] = jnp.broadcast_to(
        jnp.sum(pick[...] * quad[...], axis=1, keepdims=True), quad_slot.shape
    )
    degree = lax.broadcasted_iota(jnp.int32, (degrees, channels), 0)
    lax.fori_loop(1, n, wait_moment, 0)
    totals = jnp.sum(sums[...], axis=0)
    mean = totals[0:1] / points
    variance = totals[1:2] / points - mean * mean
    gain[...] = gain[...] * lax.rsqrt(variance + 1e-05)
    cuts = sorted({0, (ready + 1) // 2, ready, slots})
    pieces = [(b, 0, slots) for b in range(blocks - 1)]
    pieces += [(blocks - 1, first, end) for first, end in zip(cuts[:-1], cuts[1:])]

    def landing(p):
        b, first, end = pieces[p]
        if b < blocks - 1:
            return early.at[b, me]
        if first < ready:
            return late.at[me, pl.ds(first, end - first)]
        return last.at[me]

    def leaving(p, other):
        b, first, end = pieces[p]
        return outgoing.at[b, other, pl.ds(first, end - first)]

    def return_copy(p, i):
        other = lax.rem(me + i, n)
        return pltpu.make_async_remote_copy(
            src_ref=leaving(p, other), dst_ref=landing(p),
            send_sem=back_send.at[p, i], recv_sem=back_arrive.at[p, i],
            device_id={axis: other}, device_id_type=pl.DeviceIdType.MESH,
        )

    def return_own(p):
        return pltpu.make_async_copy(leaving(p, me), landing(p), back_own.at[p])

    for b in range(blocks):
        count = min(BLOCK, share - b * BLOCK)
        if count < BLOCK:
            result[...] = jnp.zeros_like(result)

        def wait_block(i, carry):
            block_copy(b, i).wait()
            return carry

        lax.fori_loop(1, n, wait_block, 0)
        own_copy(b).wait()

        def widen(i, carry):
            for s in range(slots):
                wide = recv[b, i, s].astype(F32)
                begin = pl.multiple_of((i * slots + s) * 2 * BLOCK, 8)
                for h in range(halves):
                    gathered[h, pl.ds(begin, 2 * BLOCK), :] = wide[:, h * 128 : (h + 1) * 128]
            return carry

        lax.fori_loop(0, n, widen, 0)

        def wave_step(r, carry):
            wave = owner[me * share + b * BLOCK + r]
            expanded = jnp.dot(
                pick[...].astype(BF16), legendre[b * BLOCK + r], preferred_element_type=F32
            ).astype(BF16)
            flag = jnp.where(wave == 0, 1.0, 0.0).astype(F32)
            parts = []
            for t in range(2):
                for h in range(halves):
                    lanes = slice(h * 128, (h + 1) * 128)
                    piece = gathered[h, pl.ds(t * BLOCK + r, everything, stride=2 * BLOCK), :]
                    if t == 0:
                        rest = gathered[h, pl.ds(BLOCK + r, everything, stride=2 * BLOCK), :]
                        piece = piece + rest * flag
                    else:
                        piece = piece * (1.0 - flag)
                    piece = piece - mean[:, lanes] * row_sum[t * waves + wave]
                    parts.append((piece * quad_slot[...]).astype(BF16))
            weighted = jnp.concatenate(parts, axis=1)
            coefficient = lax.dot_general(
                expanded, weighted, (((0,), (0,)), ((), ())), preferred_element_type=F32
            )
            kept = degree >= wave
            factor = jnp.where(wave > 0, 2.0, 1.0).astype(F32)
            mixed = []
            for t in range(2):
                part = coefficient[:, t * channels : (t + 1) * channels] * gain[...]
                part = jnp.where(kept, part, 0.0).astype(BF16)
                mixed.append(jnp.dot(part, mix[...], preferred_element_type=F32).astype(BF16))
            synthesis = jnp.dot(
                expanded, jnp.concatenate(mixed, axis=1), preferred_element_type=F32
            ) * factor
            for t in range(2):
                for h in range(halves):
                    begin = t * channels + h * 128
                    result[h, pl.ds(t * BLOCK + r, everything, stride=2 * BLOCK), :] = synthesis[
                        :, begin : begin + 128
                    ]
            return carry

        lax.fori_loop(0, count, wave_step, 0)

        def narrow(i, carry):
            for s in range(slots):
                begin = pl.multiple_of((i * slots + s) * 2 * BLOCK, 8)
                outgoing[b, i, s] = jnp.concatenate(
                    [result[h, pl.ds(begin, 2 * BLOCK), :] for h in range(halves)], axis=1
                ).astype(BF16)
            return carry

        lax.fori_loop(0, n, narrow, 0)

        for p in range(len(pieces)):
            if pieces[p][0] == b:

                def start_return(i, carry):
                    return_copy(p, i).start()
                    return carry

                lax.fori_loop(1, n, start_return, 0)
                return_own(p).start()

    def settle(p):
        def wait_return(i, carry):
            return_copy(p, i).wait()
            return carry

        lax.fori_loop(1, n, wait_return, 0)
        return_own(p).wait()

    def front_part(s):
        if blocks == 1:
            return jnp.zeros(partial.shape[1:], F32)
        block = early[:, :, s].reshape(split, channels)
        return jnp.dot(front[...], block, preferred_element_type=F32)

    def front_slot(s, carry):
        partial[s] = front_part(s).astype(BF16)
        return carry

    def whole_slot(s, carry):
        block = late[:, s].reshape(lines, channels)
        total = jnp.dot(back_table[...], block, preferred_element_type=F32)
        partial[s] = (front_part(s) + total).astype(BF16)
        return carry

    for p in range(blocks - 1):
        settle(p)
    lax.fori_loop(ready, slots, front_slot, 0)
    for p in range(blocks - 1, len(pieces)):
        settle(p)
        if pieces[p][1] < ready:
            lax.fori_loop(pieces[p][1], pieces[p][2], whole_slot, 0)


def inverse_kernel(last, table, partial, out, held, store):
    slots = partial.shape[0]
    ready = slots - last.shape[1]

    def store_ready(s):
        return pltpu.make_async_copy(partial.at[s], out.at[s], store.at[s])

    def store_slot(s):
        return pltpu.make_async_copy(held.at[s], out.at[ready + s], store.at[ready + s])

    def start_ready(s, carry):
        store_ready(s).start()
        return carry

    def wait_ready(s, carry):
        store_ready(s).wait()
        return carry

    def finish_slot(s, carry):
        block = last[:, s].reshape(table.shape[1], last.shape[-1])
        total = jnp.dot(table[...], block, preferred_element_type=F32)
        held[s] = (partial[ready + s].astype(F32) + total).astype(BF16)
        store_slot(s).start()
        return carry

    def wait_store(s, carry):
        store_slot(s).wait()
        return carry

    lax.fori_loop(0, ready, start_ready, 0)
    lax.fori_loop(0, slots - ready, finish_slot, 0)
    lax.fori_loop(0, ready, wait_ready, 0)
    lax.fori_loop(0, slots - ready, wait_store, 0)


def body(
    n, grid_values, lat_counts, owner_wavenumber, legendre, quad_weight, spectral_gain, channel_mix
):
    slots, longitudes, channels = grid_values.shape
    waves = owner_wavenumber.shape[0]
    share, live_total, degrees = legendre.shape
    blocks = -(-share // BLOCK)
    padded = blocks * BLOCK
    everything = n * slots
    trig = trig_table(waves, longitudes)
    base = jnp.asarray(trig)
    row_sum = jnp.asarray(trig.astype(np.float64).sum(axis=1).astype(np.float32))

    vmem = pl.BlockSpec(memory_space=pltpu.VMEM)
    smem = pl.BlockSpec(memory_space=pltpu.SMEM)
    anywhere = pl.BlockSpec(memory_space=pl.ANY)
    limit = 48 * 1024 * 1024
    packet = (blocks, n, slots, 2 * BLOCK, channels)
    copies = pltpu.SemaphoreType.DMA
    lines = n * 2 * BLOCK
    tail = min(TAIL, slots)
    returns = blocks + 2
    last, back_table, partial = pl.pallas_call(
        functools.partial(spectral_kernel, "lat", n, live_total * longitudes, share),
        out_shape=(
            pltpu.VMEM((n, tail) + packet[3:], BF16),
            pltpu.VMEM((longitudes, lines), BF16),
            pltpu.VMEM((slots, longitudes, channels), BF16),
        ),
        in_specs=[smem, smem, smem, anywhere, anywhere, anywhere, vmem, anywhere, vmem],
        out_specs=(vmem, vmem, vmem),
        scratch_shapes=[
            pltpu.VMEM((n, 2, channels), F32),
            pltpu.VMEM((n * padded, channels), F32),
            pltpu.VMEM((n * padded, waves), F32),
            pltpu.VMEM((blocks * lines, longitudes), BF16),
            pltpu.VMEM((longitudes, max(blocks - 1, 1) * lines), BF16),
            pltpu.VMEM(packet, BF16),
            pltpu.VMEM(packet, BF16),
            pltpu.VMEM((channels // 128, everything * 2 * BLOCK, 128), F32),
            pltpu.VMEM((everything, live_total), F32),
            pltpu.VMEM((everything, 128), F32),
            pltpu.VMEM(packet, BF16),
            pltpu.VMEM((channels // 128, everything * 2 * BLOCK, 128), F32),
            pltpu.VMEM((max(blocks - 1, 1),) + packet[1:], BF16),
            pltpu.VMEM((n, max(slots - tail, 1)) + packet[3:], BF16),
            pltpu.VMEM(base.shape, BF16),
            pltpu.VMEM(legendre.shape, BF16),
            pltpu.VMEM(spectral_gain.shape, F32),
            copies((slots,)), copies((3,)),
            copies((n,)), copies((n,)),
            copies((blocks, n)), copies((blocks, n)), copies((blocks,)),
            copies((returns, n)), copies((returns, n)), copies((returns,)),
        ],
        compiler_params=pltpu.CompilerParams(
            collective_id=0, has_side_effects=True, vmem_limit_bytes=limit
        ),
    )(
        lat_counts, owner_wavenumber, row_sum, grid_values, base, legendre,
        quad_weight.reshape(1, live_total), spectral_gain, channel_mix,
    )

    return pl.pallas_call(
        inverse_kernel,
        out_shape=jax.ShapeDtypeStruct((slots, longitudes, channels), BF16),
        in_specs=[vmem, vmem, vmem],
        out_specs=anywhere,
        scratch_shapes=[
            pltpu.VMEM((tail, longitudes, channels), BF16),
            copies((slots,)),
        ],
        compiler_params=pltpu.CompilerParams(vmem_limit_bytes=16 * 1024 * 1024),
    )(*[pltpu.with_memory_space_constraint(v, pltpu.VMEM) for v in (last, back_table, partial)])


def solution(mesh):
    return jax.shard_map(
        functools.partial(body, mesh.shape["lat"]),
        mesh=mesh,
        in_specs=(P(("group", "lat"), None, None), P(), P(), P("lat", None, None), P(), P(), P()),
        out_specs=P(("group", "lat"), None, None),
        check_vma=False,
    )
```

```python
import functools
import math

import jax
import jax.numpy as jnp
import numpy as np
from jax import lax
from jax.experimental import pallas as pl
from jax.experimental.pallas import tpu as pltpu
from jax.sharding import PartitionSpec as P

BLOCK = 8
TAIL = 1
F32 = jnp.float32
BF16 = jnp.bfloat16


def trig_table(waves, longitudes):
    phase = np.arange(waves)[:, None] * np.arange(longitudes)[None, :] % longitudes
    angle = phase * (2.0 * math.pi / longitudes)
    factor = 1.0 / math.sqrt(longitudes)
    table = np.concatenate([np.cos(angle) * factor, -np.sin(angle) * factor], axis=0)
    return table.astype(BF16)


def greet_all(axis, count, me):
    barrier = pltpu.get_barrier_semaphore()

    def signal(i, carry):
        other = lax.rem(me + i, count)
        pl.semaphore_signal(
            barrier, inc=1, device_id={axis: other}, device_id_type=pl.DeviceIdType.MESH
        )
        return carry

    lax.fori_loop(1, count, signal, 0)
    return barrier


def spectral_kernel(
    axis, n, points, share, counts_far, owner_far, row_sum_far, x, base_far, legendre_far,
    quad_far, gain_far, mix_far, last, back_table, partial,
    counts, owner, row_sum, quad, mix, sums, zero, hot, table, front, spec, recv, gathered, pick, quad_slot, outgoing, result,
    early, late, base, legendre, gain,
    load, fetch, mom_send, mom_recv, send, arrive, own, back_send, back_arrive, back_own,
):
    me = lax.axis_index(axis)
    slots, longitudes, channels = x.shape
    everything = n * slots
    live_total, degrees = legendre.shape[1], legendre.shape[2]
    halves = channels // 128
    blocks = spec.shape[0]
    lines = n * 2 * BLOCK
    waves = base.shape[0] // 2
    ready = slots - last.shape[1]

    def load_slot(s):
        return pltpu.make_async_copy(x.at[s], partial.at[s], load.at[s])

    def start_load(s, carry):
        load_slot(s).start()
        return carry

    base_copy = pltpu.make_async_copy(base_far, base, fetch.at[0])
    legendre_copy = pltpu.make_async_copy(legendre_far, legendre, fetch.at[1])
    gain_copy = pltpu.make_async_copy(gain_far, gain, fetch.at[2])
    owner_copy = pltpu.make_async_copy(owner_far, owner, fetch.at[3])
    counts_copy = pltpu.make_async_copy(counts_far, counts, fetch.at[4])
    row_sum_copy = pltpu.make_async_copy(row_sum_far, row_sum, fetch.at[5])
    quad_copy = pltpu.make_async_copy(quad_far, quad, fetch.at[6])
    mix_copy = pltpu.make_async_copy(mix_far, mix, fetch.at[7])
    owner_copy.start()
    base_copy.start()
    lax.fori_loop(0, slots, start_load, 0)
    counts_copy.start()
    row_sum_copy.start()
    quad_copy.start()
    mix_copy.start()
    legendre_copy.start()
    gain_copy.start()
    barrier = greet_all(axis, n, me)

    row_of = lax.broadcasted_iota(jnp.int32, (BLOCK, waves), 0)
    lane_of = lax.broadcasted_iota(jnp.int32, (BLOCK, waves), 1)

    def choose_rows(o, carry):
        for b in range(blocks):
            count = min(BLOCK, share - b * BLOCK)
            held = jnp.full((BLOCK, waves), -1, jnp.int32)
            for r in range(count):
                held = jnp.where(row_of == r, owner[o * share + b * BLOCK + r], held)
            begin = pl.multiple_of((b * n + o) * BLOCK, BLOCK)
            hot[pl.ds(begin, BLOCK), :] = jnp.where(lane_of == held, 1.0, 0.0).astype(F32)
        return carry

    owner_copy.wait()
    lax.fori_loop(0, n, choose_rows, 0)
    zero[...] = jnp.broadcast_to(hot[:, 0:1], zero.shape)
    counts_copy.wait()
    live = counts[me]
    group = math.gcd(longitudes, 32)

    def build_table(b):
        chosen = hot[b * n * BLOCK : (b + 1) * n * BLOCK, :].astype(BF16)
        both = [
            jnp.dot(chosen, base[t * waves : (t + 1) * waves], preferred_element_type=F32)
            for t in range(2)
        ]
        both = [part.reshape(n, 1, BLOCK, longitudes) for part in both]
        both = jnp.concatenate(both, axis=1).reshape(lines, longitudes)
        table[b * lines : (b + 1) * lines] = both.astype(BF16)

    def transform(b, s):
        out = jnp.dot(table[b * lines : (b + 1) * lines], partial[s], preferred_element_type=F32)
        out = out.reshape(n, 2, BLOCK, channels)
        real, imag = out[:, 0], out[:, 1]
        flag = zero[b * n * BLOCK : (b + 1) * n * BLOCK].reshape(n, BLOCK, channels)
        imag = imag + flag * (real - real.astype(BF16).astype(F32))
        out = jnp.concatenate([real, imag], axis=1)
        spec[b, :, s] = out.astype(BF16)

    def add_slot(s, carry):
        first, second = carry
        wide = partial[s].astype(F32).reshape(-1, group, channels)
        weight = jnp.where(s < live, 1.0, 0.0).astype(F32)
        first = first + weight * jnp.sum(wide, axis=0)
        second = second + weight * jnp.sum(wide * wide, axis=0)
        return first, second

    def slice_copy(b, i, first, size):
        other = lax.rem(me + i, n)
        return pltpu.make_async_remote_copy(
            src_ref=spec.at[b, other, pl.ds(first, size)],
            dst_ref=recv.at[b, me, pl.ds(first, size)],
            send_sem=send.at[b, i], recv_sem=arrive.at[b, i],
            device_id={axis: other}, device_id_type=pl.DeviceIdType.MESH,
        )

    def block_copy(b, i):
        return slice_copy(b, i, 0, slots)

    def send_slices(b, first, size):
        def start_slices(i, carry):
            slice_copy(b, i, first, size).start()
            return carry

        lax.fori_loop(1, n, start_slices, 0)

    def moment_copy(i):
        other = lax.rem(me + i, n)
        return pltpu.make_async_remote_copy(
            src_ref=sums.at[me], dst_ref=sums.at[me],
            send_sem=mom_send.at[i], recv_sem=mom_recv.at[i],
            device_id={axis: other}, device_id_type=pl.DeviceIdType.MESH,
        )

    def start_moment(i, carry):
        moment_copy(i).start()
        return carry

    def wait_moment(i, carry):
        moment_copy(i).wait()
        return carry

    def own_copy(b):
        return pltpu.make_async_copy(spec.at[b, me], recv.at[b, me], own.at[b])

    base_copy.wait()
    build_table(0)
    load_slot(0).wait()
    transform(0, 0)
    pl.semaphore_wait(barrier, n - 1)
    send_slices(0, 0, 1)

    def first_slot(s, carry):
        load_slot(s).wait()
        transform(0, s)
        return carry

    cuts = [1, 1 + (slots - 1) // 3, slots]
    for first, end in zip(cuts[:-1], cuts[1:]):
        if end > first:
            lax.fori_loop(first, end, first_slot, 0)
            send_slices(0, first, end - first)
    own_copy(0).start()
    nothing = jnp.zeros((group, channels), F32)
    first, second = lax.fori_loop(0, slots, add_slot, (nothing, nothing))
    sums[me, 0:1, :] = jnp.sum(first, axis=0, keepdims=True)
    sums[me, 1:2, :] = jnp.sum(second, axis=0, keepdims=True)
    lax.fori_loop(1, n, start_moment, 0)
    for b in range(1, blocks):
        build_table(b)

        def slot_step(s, carry):
            transform(b, s)
            return carry

        lax.fori_loop(0, slots, slot_step, 0)
        send_slices(b, 0, slots)
        own_copy(b).start()

    split = (blocks - 1) * lines
    back_table[...] = table[split:].T
    if blocks > 1:
        front[...] = table[:split].T
    legendre_copy.wait()
    gain_copy.wait()
    row_sum_copy.wait()
    quad_copy.wait()
    mix_copy.wait()
    row = lax.broadcasted_iota(jnp.int32, (everything, live_total), 0)
    lane = lax.broadcasted_iota(jnp.int32, (everything, live_total), 1)
    pick[...] = jnp.zeros_like(pick)

    def mark(i, begin):
        within = row - i * slots
        hit = (within >= 0) & (within < counts[i]) & (lane == begin + within)
        pick[...] += jnp.where(hit, 1.0, 0.0).astype(F32)
        return begin + counts[i]

    lax.fori_loop(0, n, mark, jnp.int32(0))
    quad_slot[...] = jnp.broadcast_to(
        jnp.sum(pick[...] * quad[...], axis=1, keepdims=True), quad_slot.shape
    )
    degree = lax.broadcasted_iota(jnp.int32, (degrees, channels), 0)
    lax.fori_loop(1, n, wait_moment, 0)
    totals = jnp.sum(sums[...], axis=0)
    mean = totals[0:1] / points
    variance = totals[1:2] / points - mean * mean
    gain[...] = gain[...] * lax.rsqrt(variance + 1e-05)
    cuts = sorted({0, (ready + 1) // 2, ready, slots})
    pieces = [(b, 0, slots) for b in range(blocks - 1)]
    pieces += [(blocks - 1, first, end) for first, end in zip(cuts[:-1], cuts[1:])]

    def landing(p):
        b, first, end = pieces[p]
        if b < blocks - 1:
            return early.at[b, me]
        if first < ready:
            return late.at[me, pl.ds(first, end - first)]
        return last.at[me]

    def leaving(p, other):
        b, first, end = pieces[p]
        return outgoing.at[b, other, pl.ds(first, end - first)]

    def return_copy(p, i):
        other = lax.rem(me + i, n)
        return pltpu.make_async_remote_copy(
            src_ref=leaving(p, other), dst_ref=landing(p),
            send_sem=back_send.at[p, i], recv_sem=back_arrive.at[p, i],
            device_id={axis: other}, device_id_type=pl.DeviceIdType.MESH,
        )

    def return_own(p):
        return pltpu.make_async_copy(leaving(p, me), landing(p), back_own.at[p])

    for b in range(blocks):
        count = min(BLOCK, share - b * BLOCK)
        if count < BLOCK:
            result[...] = jnp.zeros_like(result)

        def wait_block(i, carry):
            block_copy(b, i).wait()
            return carry

        lax.fori_loop(1, n, wait_block, 0)
        own_copy(b).wait()

        def widen(i, carry):
            for s in range(slots):
                wide = recv[b, i, s].astype(F32)
                begin = pl.multiple_of((i * slots + s) * 2 * BLOCK, 8)
                for h in range(halves):
                    gathered[h, pl.ds(begin, 2 * BLOCK), :] = wide[:, h * 128 : (h + 1) * 128]
            return carry

        lax.fori_loop(0, n, widen, 0)

        def wave_step(r, carry):
            wave = owner[me * share + b * BLOCK + r]
            expanded = jnp.dot(
                pick[...].astype(BF16), legendre[b * BLOCK + r], preferred_element_type=F32
            ).astype(BF16)
            flag = jnp.where(wave == 0, 1.0, 0.0).astype(F32)
            parts = []
            for t in range(2):
                for h in range(halves):
                    lanes = slice(h * 128, (h + 1) * 128)
                    piece = gathered[h, pl.ds(t * BLOCK + r, everything, stride=2 * BLOCK), :]
                    if t == 0:
                        rest = gathered[h, pl.ds(BLOCK + r, everything, stride=2 * BLOCK), :]
                        piece = piece + rest * flag
                    else:
                        piece = piece * (1.0 - flag)
                    piece = piece - mean[:, lanes] * row_sum[t * waves + wave]
                    parts.append((piece * quad_slot[...]).astype(BF16))
            weighted = jnp.concatenate(parts, axis=1)
            coefficient = lax.dot_general(
                expanded, weighted, (((0,), (0,)), ((), ())), preferred_element_type=F32
            )
            kept = degree >= wave
            factor = jnp.where(wave > 0, 2.0, 1.0).astype(F32)
            mixed = []
            for t in range(2):
                part = coefficient[:, t * channels : (t + 1) * channels] * gain[...]
                part = jnp.where(kept, part, 0.0).astype(BF16)
                mixed.append(jnp.dot(part, mix[...], preferred_element_type=F32).astype(BF16))
            synthesis = jnp.dot(
                expanded, jnp.concatenate(mixed, axis=1), preferred_element_type=F32
            ) * factor
            for t in range(2):
                for h in range(halves):
                    begin = t * channels + h * 128
                    result[h, pl.ds(t * BLOCK + r, everything, stride=2 * BLOCK), :] = synthesis[
                        :, begin : begin + 128
                    ]
            return carry

        lax.fori_loop(0, count, wave_step, 0)

        def narrow(i, carry):
            for s in range(slots):
                begin = pl.multiple_of((i * slots + s) * 2 * BLOCK, 8)
                outgoing[b, i, s] = jnp.concatenate(
                    [result[h, pl.ds(begin, 2 * BLOCK), :] for h in range(halves)], axis=1
                ).astype(BF16)
            return carry

        lax.fori_loop(0, n, narrow, 0)

        for p in range(len(pieces)):
            if pieces[p][0] == b:

                def start_return(i, carry):
                    return_copy(p, i).start()
                    return carry

                lax.fori_loop(1, n, start_return, 0)
                return_own(p).start()

    def settle(p):
        def wait_return(i, carry):
            return_copy(p, i).wait()
            return carry

        lax.fori_loop(1, n, wait_return, 0)
        return_own(p).wait()

    def front_part(s):
        if blocks == 1:
            return jnp.zeros(partial.shape[1:], F32)
        block = early[:, :, s].reshape(split, channels)
        return jnp.dot(front[...], block, preferred_element_type=F32)

    def front_slot(s, carry):
        partial[s] = front_part(s).astype(BF16)
        return carry

    def whole_slot(s, carry):
        block = late[:, s].reshape(lines, channels)
        total = jnp.dot(back_table[...], block, preferred_element_type=F32)
        partial[s] = (front_part(s) + total).astype(BF16)
        return carry

    for p in range(blocks - 1):
        settle(p)
    lax.fori_loop(ready, slots, front_slot, 0)
    for p in range(blocks - 1, len(pieces)):
        settle(p)
        if pieces[p][1] < ready:
            lax.fori_loop(pieces[p][1], pieces[p][2], whole_slot, 0)


def inverse_kernel(last, table, partial, out, held, store):
    slots = partial.shape[0]
    ready = slots - last.shape[1]

    def store_ready(s):
        return pltpu.make_async_copy(partial.at[s], out.at[s], store.at[s])

    def store_slot(s):
        return pltpu.make_async_copy(held.at[s], out.at[ready + s], store.at[ready + s])

    def start_ready(s, carry):
        store_ready(s).start()
        return carry

    def wait_ready(s, carry):
        store_ready(s).wait()
        return carry

    def finish_slot(s, carry):
        block = last[:, s].reshape(table.shape[1], last.shape[-1])
        total = jnp.dot(table[...], block, preferred_element_type=F32)
        held[s] = (partial[ready + s].astype(F32) + total).astype(BF16)
        store_slot(s).start()
        return carry

    def wait_store(s, carry):
        store_slot(s).wait()
        return carry

    lax.fori_loop(0, ready, start_ready, 0)
    lax.fori_loop(0, slots - ready, finish_slot, 0)
    lax.fori_loop(0, ready, wait_ready, 0)
    lax.fori_loop(0, slots - ready, wait_store, 0)


def body(
    n, grid_values, lat_counts, owner_wavenumber, legendre, quad_weight, spectral_gain, channel_mix
):
    slots, longitudes, channels = grid_values.shape
    waves = owner_wavenumber.shape[0]
    share, live_total, degrees = legendre.shape
    blocks = -(-share // BLOCK)
    padded = blocks * BLOCK
    everything = n * slots
    trig = trig_table(waves, longitudes)
    base = jnp.asarray(trig)
    row_sum = jnp.asarray(trig.astype(np.float64).sum(axis=1).astype(np.float32))

    vmem = pl.BlockSpec(memory_space=pltpu.VMEM)
    anywhere = pl.BlockSpec(memory_space=pl.ANY)
    limit = 48 * 1024 * 1024
    far = functools.partial(pltpu.with_memory_space_constraint, memory_space=pltpu.HBM)
    packet = (blocks, n, slots, 2 * BLOCK, channels)
    copies = pltpu.SemaphoreType.DMA
    lines = n * 2 * BLOCK
    tail = min(TAIL, slots)
    returns = blocks + 2
    last, back_table, partial = pl.pallas_call(
        functools.partial(spectral_kernel, "lat", n, live_total * longitudes, share),
        out_shape=(
            pltpu.VMEM((n, tail) + packet[3:], BF16),
            pltpu.VMEM((longitudes, lines), BF16),
            pltpu.VMEM((slots, longitudes, channels), BF16),
        ),
        in_specs=[anywhere] * 9,
        out_specs=(vmem, vmem, vmem),
        scratch_shapes=[
            pltpu.SMEM(lat_counts.shape, jnp.int32),
            pltpu.SMEM(owner_wavenumber.shape, jnp.int32),
            pltpu.SMEM(row_sum.shape, F32),
            pltpu.VMEM((1, live_total), F32),
            pltpu.VMEM(channel_mix.shape, BF16),
            pltpu.VMEM((n, 2, channels), F32),
            pltpu.VMEM((n * padded, channels), F32),
            pltpu.VMEM((n * padded, waves), F32),
            pltpu.VMEM((blocks * lines, longitudes), BF16),
            pltpu.VMEM((longitudes, max(blocks - 1, 1) * lines), BF16),
            pltpu.VMEM(packet, BF16),
            pltpu.VMEM(packet, BF16),
            pltpu.VMEM((channels // 128, everything * 2 * BLOCK, 128), F32),
            pltpu.VMEM((everything, live_total), F32),
            pltpu.VMEM((everything, 128), F32),
            pltpu.VMEM(packet, BF16),
            pltpu.VMEM((channels // 128, everything * 2 * BLOCK, 128), F32),
            pltpu.VMEM((max(blocks - 1, 1),) + packet[1:], BF16),
            pltpu.VMEM((n, max(slots - tail, 1)) + packet[3:], BF16),
            pltpu.VMEM(base.shape, BF16),
            pltpu.VMEM(legendre.shape, BF16),
            pltpu.VMEM(spectral_gain.shape, F32),
            copies((slots,)), copies((8,)),
            copies((n,)), copies((n,)),
            copies((blocks, n)), copies((blocks, n)), copies((blocks,)),
            copies((returns, n)), copies((returns, n)), copies((returns,)),
        ],
        compiler_params=pltpu.CompilerParams(
            collective_id=0, has_side_effects=True, vmem_limit_bytes=limit
        ),
    )(
        *map(far, (
            lat_counts, owner_wavenumber, row_sum, grid_values, base, legendre,
            quad_weight.reshape(1, live_total), spectral_gain, channel_mix,
        ))
    )

    return pl.pallas_call(
        inverse_kernel,
        out_shape=jax.ShapeDtypeStruct((slots, longitudes, channels), BF16),
        in_specs=[vmem, vmem, vmem],
        out_specs=anywhere,
        scratch_shapes=[
            pltpu.VMEM((tail, longitudes, channels), BF16),
            copies((slots,)),
        ],
        compiler_params=pltpu.CompilerParams(vmem_limit_bytes=16 * 1024 * 1024),
    )(*[pltpu.with_memory_space_constraint(v, pltpu.VMEM) for v in (last, back_table, partial)])


def solution(mesh):
    return jax.shard_map(
        functools.partial(body, mesh.shape["lat"]),
        mesh=mesh,
        in_specs=(P(("group", "lat"), None, None), P(), P(), P("lat", None, None), P(), P(), P()),
        out_specs=P(("group", "lat"), None, None),
        check_vma=False,
    )
```

```python
import functools
import math

import jax
import jax.numpy as jnp
import numpy as np
from jax import lax
from jax.experimental import pallas as pl
from jax.experimental.pallas import tpu as pltpu
from jax.sharding import PartitionSpec as P

BLOCK = 8
FIRST = 2
F32 = jnp.float32
BF16 = jnp.bfloat16


def trig_table(waves, longitudes):
    phase = np.arange(waves)[:, None] * np.arange(longitudes)[None, :] % longitudes
    angle = phase * (2.0 * math.pi / longitudes)
    factor = 1.0 / math.sqrt(longitudes)
    table = np.concatenate([np.cos(angle) * factor, -np.sin(angle) * factor], axis=0)
    return table.astype(BF16)


def greet_all(axis, count, me):
    barrier = pltpu.get_barrier_semaphore()

    def signal(i, carry):
        other = lax.rem(me + i, count)
        pl.semaphore_signal(
            barrier, inc=1, device_id={axis: other}, device_id_type=pl.DeviceIdType.MESH
        )
        return carry

    lax.fori_loop(1, count, signal, 0)
    return barrier


def spectral_kernel(
    axis, n, points, share, counts_far, owner_far, row_sum_far, x, base_far, legendre_far,
    quad_far, gain_far, mix_far, last, back_table, partial,
    counts, owner, row_sum, quad, mix, sums, zero, hot, table, front, spec, recv, gathered, pick, quad_slot, outgoing, result,
    early, base, legendre, gain,
    load, fetch, mom_send, mom_recv, send, arrive, own, back_send, back_arrive, back_own,
):
    me = lax.axis_index(axis)
    slots, longitudes, channels = x.shape
    everything = n * slots
    live_total, degrees = legendre.shape[1], legendre.shape[2]
    halves = channels // 128
    blocks = spec.shape[0]
    lines = n * 2 * BLOCK
    waves = base.shape[0] // 2

    def load_slot(s):
        return pltpu.make_async_copy(x.at[s], partial.at[s], load.at[s])

    def start_load(s, carry):
        load_slot(s).start()
        return carry

    base_copy = pltpu.make_async_copy(base_far, base, fetch.at[0])
    legendre_copy = pltpu.make_async_copy(legendre_far, legendre, fetch.at[1])
    gain_copy = pltpu.make_async_copy(gain_far, gain, fetch.at[2])
    owner_copy = pltpu.make_async_copy(owner_far, owner, fetch.at[3])
    counts_copy = pltpu.make_async_copy(counts_far, counts, fetch.at[4])
    row_sum_copy = pltpu.make_async_copy(row_sum_far, row_sum, fetch.at[5])
    quad_copy = pltpu.make_async_copy(quad_far, quad, fetch.at[6])
    mix_copy = pltpu.make_async_copy(mix_far, mix, fetch.at[7])
    owner_copy.start()
    base_copy.start()
    lax.fori_loop(0, slots, start_load, 0)
    counts_copy.start()
    row_sum_copy.start()
    quad_copy.start()
    mix_copy.start()
    legendre_copy.start()
    gain_copy.start()
    barrier = greet_all(axis, n, me)

    row_of = lax.broadcasted_iota(jnp.int32, (BLOCK, waves), 0)
    lane_of = lax.broadcasted_iota(jnp.int32, (BLOCK, waves), 1)

    def choose_rows(o, carry):
        for b in range(blocks):
            count = min(BLOCK, share - b * BLOCK)
            held = jnp.full((BLOCK, waves), -1, jnp.int32)
            for r in range(count):
                held = jnp.where(row_of == r, owner[o * share + b * BLOCK + r], held)
            begin = pl.multiple_of((b * n + o) * BLOCK, BLOCK)
            hot[pl.ds(begin, BLOCK), :] = jnp.where(lane_of == held, 1.0, 0.0).astype(F32)
        return carry

    owner_copy.wait()
    lax.fori_loop(0, n, choose_rows, 0)
    zero[...] = jnp.broadcast_to(hot[:, 0:1], zero.shape)
    counts_copy.wait()
    live = counts[me]
    group = math.gcd(longitudes, 32)

    def build_table(b):
        chosen = hot[b * n * BLOCK : (b + 1) * n * BLOCK, :].astype(BF16)
        both = [
            jnp.dot(chosen, base[t * waves : (t + 1) * waves], preferred_element_type=F32)
            for t in range(2)
        ]
        both = [part.reshape(n, 1, BLOCK, longitudes) for part in both]
        both = jnp.concatenate(both, axis=1).reshape(lines, longitudes)
        table[b * lines : (b + 1) * lines] = both.astype(BF16)

    def transform(b, s):
        out = jnp.dot(table[b * lines : (b + 1) * lines], partial[s], preferred_element_type=F32)
        out = out.reshape(n, 2, BLOCK, channels)
        real, imag = out[:, 0], out[:, 1]
        flag = zero[b * n * BLOCK : (b + 1) * n * BLOCK].reshape(n, BLOCK, channels)
        imag = imag + flag * (real - real.astype(BF16).astype(F32))
        out = jnp.concatenate([real, imag], axis=1)
        spec[b, :, s] = out.astype(BF16)

    def add_slot(s, carry):
        first, second = carry
        wide = partial[s].astype(F32).reshape(-1, group, channels)
        weight = jnp.where(s < live, 1.0, 0.0).astype(F32)
        first = first + weight * jnp.sum(wide, axis=0)
        second = second + weight * jnp.sum(wide * wide, axis=0)
        return first, second

    def slice_copy(b, i, first, size):
        other = lax.rem(me + i, n)
        return pltpu.make_async_remote_copy(
            src_ref=spec.at[b, other, pl.ds(first, size)],
            dst_ref=recv.at[b, me, pl.ds(first, size)],
            send_sem=send.at[b, i], recv_sem=arrive.at[b, i],
            device_id={axis: other}, device_id_type=pl.DeviceIdType.MESH,
        )

    def block_copy(b, i):
        return slice_copy(b, i, 0, slots)

    def send_slices(b, first, size):
        def start_slices(i, carry):
            slice_copy(b, i, first, size).start()
            return carry

        lax.fori_loop(1, n, start_slices, 0)

    def moment_copy(i):
        other = lax.rem(me + i, n)
        return pltpu.make_async_remote_copy(
            src_ref=sums.at[me], dst_ref=sums.at[me],
            send_sem=mom_send.at[i], recv_sem=mom_recv.at[i],
            device_id={axis: other}, device_id_type=pl.DeviceIdType.MESH,
        )

    def start_moment(i, carry):
        moment_copy(i).start()
        return carry

    def wait_moment(i, carry):
        moment_copy(i).wait()
        return carry

    def own_copy(b):
        return pltpu.make_async_copy(spec.at[b, me], recv.at[b, me], own.at[b])

    base_copy.wait()
    build_table(0)

    def first_slot(s, carry):
        load_slot(s).wait()
        transform(0, s)
        return carry

    opening = min(FIRST, slots)
    lax.fori_loop(0, opening, first_slot, 0)
    pl.semaphore_wait(barrier, n - 1)
    send_slices(0, 0, opening)
    if opening < slots:
        lax.fori_loop(opening, slots, first_slot, 0)
        send_slices(0, opening, slots - opening)
    own_copy(0).start()
    nothing = jnp.zeros((group, channels), F32)
    first, second = lax.fori_loop(0, slots, add_slot, (nothing, nothing))
    sums[me, 0:1, :] = jnp.sum(first, axis=0, keepdims=True)
    sums[me, 1:2, :] = jnp.sum(second, axis=0, keepdims=True)
    lax.fori_loop(1, n, start_moment, 0)
    for b in range(1, blocks):
        build_table(b)

        def slot_step(s, carry):
            transform(b, s)
            return carry

        lax.fori_loop(0, slots, slot_step, 0)
        send_slices(b, 0, slots)
        own_copy(b).start()

    split = (blocks - 1) * lines
    back_table[...] = table[split:].T
    if blocks > 1:
        front[...] = table[:split].T
    legendre_copy.wait()
    gain_copy.wait()
    row_sum_copy.wait()
    quad_copy.wait()
    mix_copy.wait()
    row = lax.broadcasted_iota(jnp.int32, (everything, live_total), 0)
    lane = lax.broadcasted_iota(jnp.int32, (everything, live_total), 1)
    pick[...] = jnp.zeros_like(pick)

    def mark(i, begin):
        within = row - i * slots
        hit = (within >= 0) & (within < counts[i]) & (lane == begin + within)
        pick[...] += jnp.where(hit, 1.0, 0.0).astype(F32)
        return begin + counts[i]

    lax.fori_loop(0, n, mark, jnp.int32(0))
    quad_slot[...] = jnp.broadcast_to(
        jnp.sum(pick[...] * quad[...], axis=1, keepdims=True), quad_slot.shape
    )
    degree = lax.broadcasted_iota(jnp.int32, (degrees, channels), 0)
    lax.fori_loop(1, n, wait_moment, 0)
    totals = jnp.sum(sums[...], axis=0)
    mean = totals[0:1] / points
    variance = totals[1:2] / points - mean * mean
    gain[...] = gain[...] * lax.rsqrt(variance + 1e-05)
    def landing(b):
        return early.at[b, me] if b < blocks - 1 else last.at[me]

    def return_copy(b, i):
        other = lax.rem(me + i, n)
        return pltpu.make_async_remote_copy(
            src_ref=outgoing.at[b, other], dst_ref=landing(b),
            send_sem=back_send.at[b, i], recv_sem=back_arrive.at[b, i],
            device_id={axis: other}, device_id_type=pl.DeviceIdType.MESH,
        )

    def return_own(b):
        return pltpu.make_async_copy(outgoing.at[b, me], landing(b), back_own.at[b])

    for b in range(blocks):
        count = min(BLOCK, share - b * BLOCK)
        if count < BLOCK:
            result[...] = jnp.zeros_like(result)

        def wait_block(i, carry):
            block_copy(b, i).wait()
            return carry

        lax.fori_loop(1, n, wait_block, 0)
        own_copy(b).wait()

        def widen(i, carry):
            for s in range(slots):
                wide = recv[b, i, s].astype(F32)
                begin = pl.multiple_of((i * slots + s) * 2 * BLOCK, 8)
                for h in range(halves):
                    gathered[h, pl.ds(begin, 2 * BLOCK), :] = wide[:, h * 128 : (h + 1) * 128]
            return carry

        lax.fori_loop(0, n, widen, 0)

        def wave_step(r, carry):
            wave = owner[me * share + b * BLOCK + r]
            expanded = jnp.dot(
                pick[...].astype(BF16), legendre[b * BLOCK + r], preferred_element_type=F32
            ).astype(BF16)
            flag = jnp.where(wave == 0, 1.0, 0.0).astype(F32)
            parts = []
            for t in range(2):
                for h in range(halves):
                    lanes = slice(h * 128, (h + 1) * 128)
                    piece = gathered[h, pl.ds(t * BLOCK + r, everything, stride=2 * BLOCK), :]
                    if t == 0:
                        rest = gathered[h, pl.ds(BLOCK + r, everything, stride=2 * BLOCK), :]
                        piece = piece + rest * flag
                    else:
                        piece = piece * (1.0 - flag)
                    piece = piece - mean[:, lanes] * row_sum[t * waves + wave]
                    parts.append((piece * quad_slot[...]).astype(BF16))
            weighted = jnp.concatenate(parts, axis=1)
            coefficient = lax.dot_general(
                expanded, weighted, (((0,), (0,)), ((), ())), preferred_element_type=F32
            )
            kept = degree >= wave
            factor = jnp.where(wave > 0, 2.0, 1.0).astype(F32)
            mixed = []
            for t in range(2):
                part = coefficient[:, t * channels : (t + 1) * channels] * gain[...]
                part = jnp.where(kept, part, 0.0).astype(BF16)
                mixed.append(jnp.dot(part, mix[...], preferred_element_type=F32).astype(BF16))
            synthesis = jnp.dot(
                expanded, jnp.concatenate(mixed, axis=1), preferred_element_type=F32
            ) * factor
            for t in range(2):
                for h in range(halves):
                    begin = t * channels + h * 128
                    result[h, pl.ds(t * BLOCK + r, everything, stride=2 * BLOCK), :] = synthesis[
                        :, begin : begin + 128
                    ]
            return carry

        lax.fori_loop(0, count, wave_step, 0)

        def narrow(i, carry):
            for s in range(slots):
                begin = pl.multiple_of((i * slots + s) * 2 * BLOCK, 8)
                outgoing[b, i, s] = jnp.concatenate(
                    [result[h, pl.ds(begin, 2 * BLOCK), :] for h in range(halves)], axis=1
                ).astype(BF16)
            return carry

        lax.fori_loop(0, n, narrow, 0)

        def start_return(i, carry):
            return_copy(b, i).start()
            return carry

        lax.fori_loop(1, n, start_return, 0)
        return_own(b).start()

    def settle(b):
        def wait_return(i, carry):
            return_copy(b, i).wait()
            return carry

        lax.fori_loop(1, n, wait_return, 0)
        return_own(b).wait()

    def partial_slot(s, carry):
        if blocks > 1:
            block = early[:, :, s].reshape(split, channels)
            partial[s] = jnp.dot(front[...], block, preferred_element_type=F32).astype(BF16)
        else:
            partial[s] = jnp.zeros(partial.shape[1:], BF16)
        return carry

    for b in range(blocks - 1):
        settle(b)
    lax.fori_loop(0, slots, partial_slot, 0)
    settle(blocks - 1)


def inverse_kernel(last, table, partial, out, held, store):
    slots = partial.shape[0]

    def store_slot(s):
        return pltpu.make_async_copy(held.at[s], out.at[s], store.at[s])

    for s in range(slots):
        block = last[:, s].reshape(table.shape[1], last.shape[-1])
        total = jnp.dot(table[...], block, preferred_element_type=F32)
        held[s] = (partial[s].astype(F32) + total).astype(BF16)
        store_slot(s).start()
    for s in range(slots):
        store_slot(s).wait()


def body(
    n, grid_values, lat_counts, owner_wavenumber, legendre, quad_weight, spectral_gain, channel_mix
):
    slots, longitudes, channels = grid_values.shape
    waves = owner_wavenumber.shape[0]
    share, live_total, degrees = legendre.shape
    blocks = -(-share // BLOCK)
    padded = blocks * BLOCK
    everything = n * slots
    trig = trig_table(waves, longitudes)
    base = jnp.asarray(trig)
    row_sum = jnp.asarray(trig.astype(np.float64).sum(axis=1).astype(np.float32))

    vmem = pl.BlockSpec(memory_space=pltpu.VMEM)
    anywhere = pl.BlockSpec(memory_space=pl.ANY)
    limit = 48 * 1024 * 1024
    far = functools.partial(pltpu.with_memory_space_constraint, memory_space=pltpu.HBM)
    packet = (blocks, n, slots, 2 * BLOCK, channels)
    copies = pltpu.SemaphoreType.DMA
    lines = n * 2 * BLOCK
    last, back_table, partial = pl.pallas_call(
        functools.partial(spectral_kernel, "lat", n, live_total * longitudes, share),
        out_shape=(
            pltpu.VMEM(packet[1:], BF16),
            pltpu.VMEM((longitudes, lines), BF16),
            pltpu.VMEM((slots, longitudes, channels), BF16),
        ),
        in_specs=[anywhere] * 9,
        out_specs=(vmem, vmem, vmem),
        scratch_shapes=[
            pltpu.SMEM(lat_counts.shape, jnp.int32),
            pltpu.SMEM(owner_wavenumber.shape, jnp.int32),
            pltpu.SMEM(row_sum.shape, F32),
            pltpu.VMEM((1, live_total), F32),
            pltpu.VMEM(channel_mix.shape, BF16),
            pltpu.VMEM((n, 2, channels), F32),
            pltpu.VMEM((n * padded, channels), F32),
            pltpu.VMEM((n * padded, waves), F32),
            pltpu.VMEM((blocks * lines, longitudes), BF16),
            pltpu.VMEM((longitudes, max(blocks - 1, 1) * lines), BF16),
            pltpu.VMEM(packet, BF16),
            pltpu.VMEM(packet, BF16),
            pltpu.VMEM((channels // 128, everything * 2 * BLOCK, 128), F32),
            pltpu.VMEM((everything, live_total), F32),
            pltpu.VMEM((everything, 128), F32),
            pltpu.VMEM(packet, BF16),
            pltpu.VMEM((channels // 128, everything * 2 * BLOCK, 128), F32),
            pltpu.VMEM((max(blocks - 1, 1),) + packet[1:], BF16),
            pltpu.VMEM(base.shape, BF16),
            pltpu.VMEM(legendre.shape, BF16),
            pltpu.VMEM(spectral_gain.shape, F32),
            copies((slots,)), copies((8,)),
            copies((n,)), copies((n,)),
            copies((blocks, n)), copies((blocks, n)), copies((blocks,)),
            copies((blocks, n)), copies((blocks, n)), copies((blocks,)),
        ],
        compiler_params=pltpu.CompilerParams(
            collective_id=0, has_side_effects=True, vmem_limit_bytes=limit
        ),
    )(
        *map(far, (
            lat_counts, owner_wavenumber, row_sum, grid_values, base, legendre,
            quad_weight.reshape(1, live_total), spectral_gain, channel_mix,
        ))
    )

    return pl.pallas_call(
        inverse_kernel,
        out_shape=jax.ShapeDtypeStruct((slots, longitudes, channels), BF16),
        in_specs=[vmem, vmem, vmem],
        out_specs=anywhere,
        scratch_shapes=[
            pltpu.VMEM((slots, longitudes, channels), BF16),
            copies((slots,)),
        ],
        compiler_params=pltpu.CompilerParams(vmem_limit_bytes=16 * 1024 * 1024),
    )(*[pltpu.with_memory_space_constraint(v, pltpu.VMEM) for v in (last, back_table, partial)])


def solution(mesh):
    return jax.shard_map(
        functools.partial(body, mesh.shape["lat"]),
        mesh=mesh,
        in_specs=(P(("group", "lat"), None, None), P(), P(), P("lat", None, None), P(), P(), P()),
        out_specs=P(("group", "lat"), None, None),
        check_vma=False,
    )
```

```python
import functools
import math

import jax
import jax.numpy as jnp
import numpy as np
from jax import lax
from jax.experimental import pallas as pl
from jax.experimental.pallas import tpu as pltpu
from jax.sharding import PartitionSpec as P

BLOCK = 8
FIRST = 2
TAIL = 3
HELD = 1
F32 = jnp.float32
BF16 = jnp.bfloat16


def trig_table(waves, longitudes):
    phase = np.arange(waves)[:, None] * np.arange(longitudes)[None, :] % longitudes
    angle = phase * (2.0 * math.pi / longitudes)
    factor = 1.0 / math.sqrt(longitudes)
    table = np.concatenate([np.cos(angle) * factor, -np.sin(angle) * factor], axis=0)
    return table.astype(BF16)


def homeward_pieces(blocks, slots, ready, held_back):
    pieces = [(b, 1, 0, slots) for b in range(held_back)]
    if ready > 0:
        pieces.append((held_back, blocks - held_back, 0, ready))
    pieces.append((held_back, blocks - held_back, ready, slots - ready))
    return pieces


def greet_all(axis, count, me):
    barrier = pltpu.get_barrier_semaphore()

    def signal(i, carry):
        other = lax.rem(me + i, count)
        pl.semaphore_signal(
            barrier, inc=1, device_id={axis: other}, device_id_type=pl.DeviceIdType.MESH
        )
        return carry

    lax.fori_loop(1, count, signal, 0)
    return barrier


def spectral_kernel(
    axis, n, points, share, counts_far, owner_far, row_sum_far, x, base_far, legendre_far,
    quad_far, gain_far, mix_far, last, back_table, partial,
    counts, owner, row_sum, quad, mix, halves_of, sums, zero, hot, table, front, spec, recv, gathered, pick, quad_slot, outgoing, result,
    back, base, legendre, gain,
    load, fetch, mom_send, mom_recv, send, arrive, own, back_send, back_arrive, back_own,
):
    me = lax.axis_index(axis)
    slots, longitudes, channels = x.shape
    everything = n * slots
    live_total, degrees = legendre.shape[1], legendre.shape[2]
    halves = channels // 128
    blocks = spec.shape[0]
    lines = n * 2 * BLOCK
    waves = base.shape[0] // 2
    ready, held_back = slots - last.shape[2], blocks - last.shape[0]
    homeward = homeward_pieces(blocks, slots, ready, held_back)

    def load_slot(s):
        return pltpu.make_async_copy(x.at[s], partial.at[s], load.at[s])

    def start_load(s, carry):
        load_slot(s).start()
        return carry

    base_copy = pltpu.make_async_copy(base_far, base, fetch.at[0])
    legendre_copy = pltpu.make_async_copy(legendre_far, legendre, fetch.at[1])
    gain_copy = pltpu.make_async_copy(gain_far, gain, fetch.at[2])
    owner_copy = pltpu.make_async_copy(owner_far, owner, fetch.at[3])
    counts_copy = pltpu.make_async_copy(counts_far, counts, fetch.at[4])
    row_sum_copy = pltpu.make_async_copy(row_sum_far, row_sum, fetch.at[5])
    quad_copy = pltpu.make_async_copy(quad_far, quad, fetch.at[6])
    mix_copy = pltpu.make_async_copy(mix_far, mix, fetch.at[7])
    owner_copy.start()
    opening = min(FIRST, slots)
    base_copy.start()
    lax.fori_loop(0, opening, start_load, 0)
    barrier = greet_all(axis, n, me)

    row_of = lax.broadcasted_iota(jnp.int32, (BLOCK, waves), 0)
    lane_of = lax.broadcasted_iota(jnp.int32, (BLOCK, waves), 1)

    def choose_rows(b):
        count = min(BLOCK, share - b * BLOCK)

        def choose_owner(o, carry):
            held = jnp.full((BLOCK, waves), -1, jnp.int32)
            for r in range(count):
                held = jnp.where(row_of == r, owner[o * share + b * BLOCK + r], held)
            begin = pl.multiple_of((b * n + o) * BLOCK, BLOCK)
            hit = jnp.where(lane_of == held, 1.0, 0.0).astype(F32)
            hot[pl.ds(begin, BLOCK), :] = hit
            zero[pl.ds(begin, BLOCK), :] = jnp.broadcast_to(hit[:, 0:1], (BLOCK, channels))
            return carry

        lax.fori_loop(0, n, choose_owner, 0)

    owner_copy.wait()
    choose_rows(0)
    group = math.gcd(longitudes, 32)

    def build_table(b):
        chosen = hot[b * n * BLOCK : (b + 1) * n * BLOCK, :].astype(BF16)
        both = [
            jnp.dot(chosen, base[t * waves : (t + 1) * waves], preferred_element_type=F32)
            for t in range(2)
        ]
        both = [part.reshape(n, 1, BLOCK, longitudes) for part in both]
        both = jnp.concatenate(both, axis=1).reshape(lines, longitudes)
        table[b * lines : (b + 1) * lines] = both.astype(BF16)

    def transform(b, s):
        out = jnp.dot(table[b * lines : (b + 1) * lines], partial[s], preferred_element_type=F32)
        out = out.reshape(n, 2, BLOCK, channels)
        real, imag = out[:, 0], out[:, 1]
        flag = zero[b * n * BLOCK : (b + 1) * n * BLOCK].reshape(n, BLOCK, channels)
        imag = imag + flag * (real - real.astype(BF16).astype(F32))
        out = jnp.concatenate([real, imag], axis=1)
        spec[b, :, s] = out.astype(BF16)

    def add_slot(live, s, carry):
        first, second = carry
        wide = partial[s].astype(F32).reshape(-1, group, channels)
        weight = jnp.where(s < live, 1.0, 0.0).astype(F32)
        first = first + weight * jnp.sum(wide, axis=0)
        second = second + weight * jnp.sum(wide * wide, axis=0)
        return first, second

    def slice_copy(b, i, first, size):
        other = lax.rem(me + i, n)
        return pltpu.make_async_remote_copy(
            src_ref=spec.at[b, other, pl.ds(first, size)],
            dst_ref=recv.at[b, me, pl.ds(first, size)],
            send_sem=send.at[b, i], recv_sem=arrive.at[b, i],
            device_id={axis: other}, device_id_type=pl.DeviceIdType.MESH,
        )

    def block_copy(b, i):
        return slice_copy(b, i, 0, slots)

    def send_slices(b, first, size):
        def start_slices(i, carry):
            slice_copy(b, i, first, size).start()
            return carry

        lax.fori_loop(1, n, start_slices, 0)

    pairs, pair = n // 2, me // 2

    def partner_copy():
        return pltpu.make_async_remote_copy(
            src_ref=halves_of.at[0], dst_ref=halves_of.at[1],
            send_sem=mom_send.at[0], recv_sem=mom_recv.at[0],
            device_id={axis: me + 1 - 2 * lax.rem(me, 2)},
            device_id_type=pl.DeviceIdType.MESH,
        )

    def moment_copy(i):
        other = lax.rem(me + 2 * i, n)
        return pltpu.make_async_remote_copy(
            src_ref=sums.at[pair], dst_ref=sums.at[pair],
            send_sem=mom_send.at[i], recv_sem=mom_recv.at[i],
            device_id={axis: other}, device_id_type=pl.DeviceIdType.MESH,
        )

    def start_moment(i, carry):
        moment_copy(i).start()
        return carry

    def wait_moment(i, carry):
        moment_copy(i).wait()
        return carry

    def own_copy(b):
        return pltpu.make_async_copy(spec.at[b, me], recv.at[b, me], own.at[b])

    base_copy.wait()
    lax.fori_loop(opening, slots, start_load, 0)
    counts_copy.start()
    row_sum_copy.start()
    quad_copy.start()
    mix_copy.start()
    legendre_copy.start()
    gain_copy.start()
    build_table(0)

    def first_slot(s, carry):
        load_slot(s).wait()
        transform(0, s)
        return carry

    lax.fori_loop(0, opening, first_slot, 0)
    pl.semaphore_wait(barrier, n - 1)
    send_slices(0, 0, opening)
    if opening < slots:
        lax.fori_loop(opening, slots, first_slot, 0)
        send_slices(0, opening, slots - opening)
    own_copy(0).start()
    counts_copy.wait()
    live = counts[me]
    nothing = jnp.zeros((group, channels), F32)
    first, second = lax.fori_loop(
        0, slots, functools.partial(add_slot, live), (nothing, nothing)
    )
    halves_of[0, 0:1, :] = jnp.sum(first, axis=0, keepdims=True)
    halves_of[0, 1:2, :] = jnp.sum(second, axis=0, keepdims=True)
    partner_copy().start()
    partner_copy().wait()
    sums[pair] = halves_of[0] + halves_of[1]
    lax.fori_loop(1, pairs, start_moment, 0)
    for b in range(1, blocks):
        choose_rows(b)
        build_table(b)

        def slot_step(s, carry):
            transform(b, s)
            return carry

        lax.fori_loop(0, slots, slot_step, 0)
        send_slices(b, 0, slots)
        own_copy(b).start()

    split = held_back * lines
    for b in range(blocks):
        turned = table[b * lines : (b + 1) * lines].T
        front[:, b * lines : (b + 1) * lines] = turned
        if b >= held_back:
            back_table[:, (b - held_back) * lines : (b - held_back + 1) * lines] = turned
    legendre_copy.wait()
    gain_copy.wait()
    row_sum_copy.wait()
    quad_copy.wait()
    mix_copy.wait()
    row = lax.broadcasted_iota(jnp.int32, (everything, live_total), 0)
    lane = lax.broadcasted_iota(jnp.int32, (everything, live_total), 1)
    pick[...] = jnp.zeros_like(pick)

    def mark(i, begin):
        within = row - i * slots
        hit = (within >= 0) & (within < counts[i]) & (lane == begin + within)
        pick[...] += jnp.where(hit, 1.0, 0.0).astype(F32)
        return begin + counts[i]

    lax.fori_loop(0, n, mark, jnp.int32(0))
    quad_slot[...] = jnp.broadcast_to(
        jnp.sum(pick[...] * quad[...], axis=1, keepdims=True), quad_slot.shape
    )
    degree = lax.broadcasted_iota(jnp.int32, (degrees, channels), 0)
    lax.fori_loop(1, pairs, wait_moment, 0)
    totals = jnp.sum(sums[...], axis=0)
    mean = totals[0:1] / points
    variance = totals[1:2] / points - mean * mean
    gain[...] = gain[...] * lax.rsqrt(variance + 1e-05)
    def part(ref, piece, device):
        b, many, first, size = piece
        return ref.at[pl.ds(b, many), device, pl.ds(first, size)]

    def landing(p):
        if p < len(homeward) - 1:
            return part(back, homeward[p], me)
        return last.at[:, me]

    def return_copy(p, i):
        other = lax.rem(me + i, n)
        return pltpu.make_async_remote_copy(
            src_ref=part(outgoing, homeward[p], other), dst_ref=landing(p),
            send_sem=back_send.at[p, i], recv_sem=back_arrive.at[p, i],
            device_id={axis: other}, device_id_type=pl.DeviceIdType.MESH,
        )

    def return_own(p):
        return pltpu.make_async_copy(
            part(outgoing, homeward[p], me), landing(p), back_own.at[p]
        )

    for b in range(blocks):
        count = min(BLOCK, share - b * BLOCK)
        if count < BLOCK:
            result[...] = jnp.zeros_like(result)

        def wait_block(i, carry):
            block_copy(b, i).wait()
            return carry

        lax.fori_loop(1, n, wait_block, 0)
        own_copy(b).wait()

        def widen(i, carry):
            for s in range(slots):
                wide = recv[b, i, s].astype(F32)
                begin = pl.multiple_of((i * slots + s) * 2 * BLOCK, 8)
                for h in range(halves):
                    gathered[h, pl.ds(begin, 2 * BLOCK), :] = wide[:, h * 128 : (h + 1) * 128]
            return carry

        lax.fori_loop(0, n, widen, 0)

        def wave_step(r, carry):
            wave = owner[me * share + b * BLOCK + r]
            expanded = jnp.dot(
                pick[...].astype(BF16), legendre[b * BLOCK + r], preferred_element_type=F32
            ).astype(BF16)
            flag = jnp.where(wave == 0, 1.0, 0.0).astype(F32)
            parts = []
            for t in range(2):
                for h in range(halves):
                    lanes = slice(h * 128, (h + 1) * 128)
                    piece = gathered[h, pl.ds(t * BLOCK + r, everything, stride=2 * BLOCK), :]
                    if t == 0:
                        rest = gathered[h, pl.ds(BLOCK + r, everything, stride=2 * BLOCK), :]
                        piece = piece + rest * flag
                    else:
                        piece = piece * (1.0 - flag)
                    piece = piece - mean[:, lanes] * row_sum[t * waves + wave]
                    parts.append((piece * quad_slot[...]).astype(BF16))
            weighted = jnp.concatenate(parts, axis=1)
            coefficient = lax.dot_general(
                expanded, weighted, (((0,), (0,)), ((), ())), preferred_element_type=F32
            )
            kept = degree >= wave
            factor = jnp.where(wave > 0, 2.0, 1.0).astype(F32)
            mixed = []
            for t in range(2):
                part = coefficient[:, t * channels : (t + 1) * channels] * gain[...]
                part = jnp.where(kept, part, 0.0).astype(BF16)
                mixed.append(jnp.dot(part, mix[...], preferred_element_type=F32).astype(BF16))
            synthesis = jnp.dot(
                expanded, jnp.concatenate(mixed, axis=1), preferred_element_type=F32
            ) * factor
            for t in range(2):
                for h in range(halves):
                    begin = t * channels + h * 128
                    result[h, pl.ds(t * BLOCK + r, everything, stride=2 * BLOCK), :] = synthesis[
                        :, begin : begin + 128
                    ]
            return carry

        lax.fori_loop(0, count, wave_step, 0)

        def narrow(i, carry):
            for s in range(slots):
                begin = pl.multiple_of((i * slots + s) * 2 * BLOCK, 8)
                outgoing[b, i, s] = jnp.concatenate(
                    [result[h, pl.ds(begin, 2 * BLOCK), :] for h in range(halves)], axis=1
                ).astype(BF16)
            return carry

        lax.fori_loop(0, n, narrow, 0)

        for p, piece in enumerate(homeward):
            if piece[0] + piece[1] - 1 == b:

                def start_return(i, carry):
                    return_copy(p, i).start()
                    return carry

                lax.fori_loop(1, n, start_return, 0)
                return_own(p).start()

    def settle(p):
        def wait_return(i, carry):
            return_copy(p, i).wait()
            return carry

        lax.fori_loop(1, n, wait_return, 0)
        return_own(p).wait()

    def whole_slot(s, carry):
        block = back[:, :, s].reshape(blocks * lines, channels)
        partial[s] = jnp.dot(front[...], block, preferred_element_type=F32).astype(BF16)
        return carry

    def front_slot(s, carry):
        if held_back > 0:
            block = back[:held_back, :, s].reshape(split, channels)
            total = jnp.dot(front[:, :split], block, preferred_element_type=F32)
            partial[s] = total.astype(BF16)
        else:
            partial[s] = jnp.zeros(partial.shape[1:], BF16)
        return carry

    for p in range(held_back):
        settle(p)
    lax.fori_loop(ready, slots, front_slot, 0)
    for p in range(held_back, len(homeward) - 1):
        settle(p)
        lax.fori_loop(0, ready, whole_slot, 0)
    settle(len(homeward) - 1)


def inverse_kernel(last, table, partial, out, held, store):
    slots = partial.shape[0]
    ready = slots - last.shape[2]

    def store_slot(s):
        source = partial.at[s] if s < ready else held.at[s - ready]
        return pltpu.make_async_copy(source, out.at[s], store.at[s])

    for s in range(ready):
        store_slot(s).start()
    for s in range(ready, slots):
        block = last[:, :, s - ready].reshape(table.shape[1], last.shape[-1])
        total = jnp.dot(table[...], block, preferred_element_type=F32)
        held[s - ready] = (partial[s].astype(F32) + total).astype(BF16)
        store_slot(s).start()
    for s in range(slots):
        store_slot(s).wait()


def body(
    n, grid_values, lat_counts, owner_wavenumber, legendre, quad_weight, spectral_gain, channel_mix
):
    slots, longitudes, channels = grid_values.shape
    waves = owner_wavenumber.shape[0]
    share, live_total, degrees = legendre.shape
    blocks = -(-share // BLOCK)
    padded = blocks * BLOCK
    everything = n * slots
    trig = trig_table(waves, longitudes)
    base = jnp.asarray(trig)
    row_sum = jnp.asarray(trig.astype(np.float64).sum(axis=1).astype(np.float32))

    vmem = pl.BlockSpec(memory_space=pltpu.VMEM)
    anywhere = pl.BlockSpec(memory_space=pl.ANY)
    limit = 48 * 1024 * 1024
    far = functools.partial(pltpu.with_memory_space_constraint, memory_space=pltpu.HBM)
    packet = (blocks, n, slots, 2 * BLOCK, channels)
    copies = pltpu.SemaphoreType.DMA
    lines = n * 2 * BLOCK
    tail = min(TAIL, slots)
    late = max(blocks - HELD, 1)
    returns = len(homeward_pieces(blocks, slots, slots - tail, blocks - late))
    last, back_table, partial = pl.pallas_call(
        functools.partial(spectral_kernel, "lat", n, live_total * longitudes, share),
        out_shape=(
            pltpu.VMEM((late, n, tail) + packet[3:], BF16),
            pltpu.VMEM((longitudes, late * lines), BF16),
            pltpu.VMEM((slots, longitudes, channels), BF16),
        ),
        in_specs=[anywhere] * 9,
        out_specs=(vmem, vmem, vmem),
        scratch_shapes=[
            pltpu.SMEM(lat_counts.shape, jnp.int32),
            pltpu.SMEM(owner_wavenumber.shape, jnp.int32),
            pltpu.SMEM(row_sum.shape, F32),
            pltpu.VMEM((1, live_total), F32),
            pltpu.VMEM(channel_mix.shape, BF16),
            pltpu.VMEM((2, 2, channels), F32),
            pltpu.VMEM((n // 2, 2, channels), F32),
            pltpu.VMEM((n * padded, channels), F32),
            pltpu.VMEM((n * padded, waves), F32),
            pltpu.VMEM((blocks * lines, longitudes), BF16),
            pltpu.VMEM((longitudes, blocks * lines), BF16),
            pltpu.VMEM(packet, BF16),
            pltpu.VMEM(packet, BF16),
            pltpu.VMEM((channels // 128, everything * 2 * BLOCK, 128), F32),
            pltpu.VMEM((everything, live_total), F32),
            pltpu.VMEM((everything, 128), F32),
            pltpu.VMEM(packet, BF16),
            pltpu.VMEM((channels // 128, everything * 2 * BLOCK, 128), F32),
            pltpu.VMEM(packet, BF16),
            pltpu.VMEM(base.shape, BF16),
            pltpu.VMEM(legendre.shape, BF16),
            pltpu.VMEM(spectral_gain.shape, F32),
            copies((slots,)), copies((8,)),
            copies((n // 2,)), copies((n // 2,)),
            copies((blocks, n)), copies((blocks, n)), copies((blocks,)),
            copies((returns, n)), copies((returns, n)), copies((returns,)),
        ],
        compiler_params=pltpu.CompilerParams(
            collective_id=0, has_side_effects=True, vmem_limit_bytes=limit
        ),
    )(
        *map(far, (
            lat_counts, owner_wavenumber, row_sum, grid_values, base, legendre,
            quad_weight.reshape(1, live_total), spectral_gain, channel_mix,
        ))
    )

    return pl.pallas_call(
        inverse_kernel,
        out_shape=jax.ShapeDtypeStruct((slots, longitudes, channels), BF16),
        in_specs=[vmem, vmem, vmem],
        out_specs=anywhere,
        scratch_shapes=[
            pltpu.VMEM((tail, longitudes, channels), BF16),
            copies((slots,)),
        ],
        compiler_params=pltpu.CompilerParams(vmem_limit_bytes=16 * 1024 * 1024),
    )(*[pltpu.with_memory_space_constraint(v, pltpu.VMEM) for v in (last, back_table, partial)])


def solution(mesh):
    return jax.shard_map(
        functools.partial(body, mesh.shape["lat"]),
        mesh=mesh,
        in_specs=(P(("group", "lat"), None, None), P(), P(), P("lat", None, None), P(), P(), P()),
        out_specs=P(("group", "lat"), None, None),
        check_vma=False,
    )
```

```python
import functools
import math

import jax
import jax.numpy as jnp
import numpy as np
from jax import lax
from jax.experimental import pallas as pl
from jax.experimental.pallas import tpu as pltpu
from jax.sharding import PartitionSpec as P

BLOCK = 8
FIRST = 2
TAIL = 3
HELD = 1
F32 = jnp.float32
BF16 = jnp.bfloat16


def trig_table(waves, longitudes):
    phase = np.arange(waves)[:, None] * np.arange(longitudes)[None, :] % longitudes
    angle = phase * (2.0 * math.pi / longitudes)
    factor = 1.0 / math.sqrt(longitudes)
    table = np.concatenate([np.cos(angle) * factor, -np.sin(angle) * factor], axis=0)
    return table.astype(BF16)


def homeward_pieces(blocks, slots, ready, held_back):
    pieces = [(b, 1, 0, slots) for b in range(held_back)]
    if ready > 0:
        pieces.append((held_back, blocks - held_back, 0, ready))
    pieces.append((held_back, blocks - held_back, ready, slots - ready))
    return pieces


def greet_all(axis, count, me):
    barrier = pltpu.get_barrier_semaphore()

    def signal(i, carry):
        other = lax.rem(me + i, count)
        pl.semaphore_signal(
            barrier, inc=1, device_id={axis: other}, device_id_type=pl.DeviceIdType.MESH
        )
        return carry

    lax.fori_loop(1, count, signal, 0)
    return barrier


def spectral_kernel(
    axis, n, points, share, counts_far, owner_far, row_sum_far, x, base_far, legendre_far,
    quad_far, gain_far, mix_far, last, back_table, partial,
    counts, owner, row_sum, quad, mix, halves_of, sums, zero, hot, table, front, spec, recv, gathered, pick, quad_slot, outgoing, result,
    back, base, legendre, gain,
    load, fetch, mom_send, mom_recv, send, arrive, own, back_send, back_arrive, back_own,
):
    me = lax.axis_index(axis)
    slots, longitudes, channels = x.shape
    everything = n * slots
    live_total, degrees = legendre.shape[1], legendre.shape[2]
    halves = channels // 128
    blocks = spec.shape[0]
    lines = n * 2 * BLOCK
    waves = base.shape[0] // 2
    ready, held_back = slots - last.shape[2], blocks - last.shape[0]
    homeward = homeward_pieces(blocks, slots, ready, held_back)

    def load_slot(s):
        return pltpu.make_async_copy(x.at[s], partial.at[s], load.at[s])

    def start_load(s, carry):
        load_slot(s).start()
        return carry

    base_copy = pltpu.make_async_copy(base_far, base, fetch.at[0])
    legendre_copy = pltpu.make_async_copy(legendre_far, legendre, fetch.at[1])
    gain_copy = pltpu.make_async_copy(gain_far, gain, fetch.at[2])
    owner_copy = pltpu.make_async_copy(owner_far, owner, fetch.at[3])
    counts_copy = pltpu.make_async_copy(counts_far, counts, fetch.at[4])
    row_sum_copy = pltpu.make_async_copy(row_sum_far, row_sum, fetch.at[5])
    quad_copy = pltpu.make_async_copy(quad_far, quad, fetch.at[6])
    mix_copy = pltpu.make_async_copy(mix_far, mix, fetch.at[7])
    owner_copy.start()
    opening = min(FIRST, slots)
    base_copy.start()
    lax.fori_loop(0, opening, start_load, 0)
    barrier = greet_all(axis, n, me)

    row_of = lax.broadcasted_iota(jnp.int32, (BLOCK, waves), 0)
    lane_of = lax.broadcasted_iota(jnp.int32, (BLOCK, waves), 1)

    def choose_rows(b):
        count = min(BLOCK, share - b * BLOCK)

        def choose_owner(o, carry):
            held = jnp.full((BLOCK, waves), -1, jnp.int32)
            for r in range(count):
                held = jnp.where(row_of == r, owner[o * share + b * BLOCK + r], held)
            begin = pl.multiple_of((b * n + o) * BLOCK, BLOCK)
            hit = jnp.where(lane_of == held, 1.0, 0.0).astype(F32)
            hot[pl.ds(begin, BLOCK), :] = hit
            zero[pl.ds(begin, BLOCK), :] = jnp.broadcast_to(hit[:, 0:1], (BLOCK, channels))
            return carry

        lax.fori_loop(0, n, choose_owner, 0)

    owner_copy.wait()
    choose_rows(0)
    group = math.gcd(longitudes, 32)

    def build_table(b):
        chosen = hot[b * n * BLOCK : (b + 1) * n * BLOCK, :].astype(BF16)
        both = [
            jnp.dot(chosen, base[t * waves : (t + 1) * waves], preferred_element_type=F32)
            for t in range(2)
        ]
        both = [part.reshape(n, 1, BLOCK, longitudes) for part in both]
        both = jnp.concatenate(both, axis=1).reshape(lines, longitudes)
        table[b * lines : (b + 1) * lines] = both.astype(BF16)

    def transform(b, s):
        out = jnp.dot(table[b * lines : (b + 1) * lines], partial[s], preferred_element_type=F32)
        out = out.reshape(n, 2, BLOCK, channels)
        real, imag = out[:, 0], out[:, 1]
        flag = zero[b * n * BLOCK : (b + 1) * n * BLOCK].reshape(n, BLOCK, channels)
        imag = imag + flag * (real - real.astype(BF16).astype(F32))
        out = jnp.concatenate([real, imag], axis=1)
        spec[b, :, s] = out.astype(BF16)

    def add_slot(live, s, carry):
        first, second = carry
        wide = partial[s].astype(F32).reshape(-1, group, channels)
        weight = jnp.where(s < live, 1.0, 0.0).astype(F32)
        first = first + weight * jnp.sum(wide, axis=0)
        second = second + weight * jnp.sum(wide * wide, axis=0)
        return first, second

    def slice_copy(b, i, first, size):
        other = lax.rem(me + i, n)
        return pltpu.make_async_remote_copy(
            src_ref=spec.at[b, other, pl.ds(first, size)],
            dst_ref=recv.at[b, me, pl.ds(first, size)],
            send_sem=send.at[b, i], recv_sem=arrive.at[b, i],
            device_id={axis: other}, device_id_type=pl.DeviceIdType.MESH,
        )

    def block_copy(b, i):
        return slice_copy(b, i, 0, slots)

    def send_slices(b, first, size):
        def start_slices(i, carry):
            slice_copy(b, i, first, size).start()
            return carry

        lax.fori_loop(1, n, start_slices, 0)

    pairs, pair = n // 2, me // 2

    def partner_copy():
        return pltpu.make_async_remote_copy(
            src_ref=halves_of.at[0], dst_ref=halves_of.at[1],
            send_sem=mom_send.at[0], recv_sem=mom_recv.at[0],
            device_id={axis: me + 1 - 2 * lax.rem(me, 2)},
            device_id_type=pl.DeviceIdType.MESH,
        )

    def moment_copy(i):
        other = lax.rem(me + 2 * i, n)
        return pltpu.make_async_remote_copy(
            src_ref=sums.at[pair], dst_ref=sums.at[pair],
            send_sem=mom_send.at[i], recv_sem=mom_recv.at[i],
            device_id={axis: other}, device_id_type=pl.DeviceIdType.MESH,
        )

    def start_moment(i, carry):
        moment_copy(i).start()
        return carry

    def wait_moment(i, carry):
        moment_copy(i).wait()
        return carry

    def own_copy(b):
        return pltpu.make_async_copy(spec.at[b, me], recv.at[b, me], own.at[b])

    base_copy.wait()
    lax.fori_loop(opening, slots, start_load, 0)
    counts_copy.start()
    row_sum_copy.start()
    quad_copy.start()
    mix_copy.start()
    legendre_copy.start()
    gain_copy.start()
    build_table(0)

    def first_slot(s, carry):
        load_slot(s).wait()
        transform(0, s)
        return carry

    lax.fori_loop(0, opening, first_slot, 0)
    pl.semaphore_wait(barrier, n - 1)
    send_slices(0, 0, opening)
    if opening < slots:
        lax.fori_loop(opening, slots, first_slot, 0)
        send_slices(0, opening, slots - opening)
    own_copy(0).start()
    counts_copy.wait()
    live = counts[me]
    nothing = jnp.zeros((group, channels), F32)

    def share_moments(first, second):
        halves_of[0, 0:1, :] = jnp.sum(first, axis=0, keepdims=True)
        halves_of[0, 1:2, :] = jnp.sum(second, axis=0, keepdims=True)
        partner_copy().start()
        partner_copy().wait()
        sums[pair] = halves_of[0] + halves_of[1]
        lax.fori_loop(1, pairs, start_moment, 0)

    if blocks == 1:
        share_moments(*lax.fori_loop(
            0, slots, functools.partial(add_slot, live), (nothing, nothing)
        ))
    for b in range(1, blocks):
        choose_rows(b)
        build_table(b)

        def slot_step(s, carry):
            transform(b, s)
            return add_slot(live, s, carry) if b == 1 else carry

        totals = lax.fori_loop(0, slots, slot_step, (nothing, nothing))
        send_slices(b, 0, slots)
        own_copy(b).start()
        if b == 1:
            share_moments(*totals)

    split = held_back * lines
    for b in range(blocks):
        turned = table[b * lines : (b + 1) * lines].T
        front[:, b * lines : (b + 1) * lines] = turned
        if b >= held_back:
            back_table[:, (b - held_back) * lines : (b - held_back + 1) * lines] = turned
    legendre_copy.wait()
    gain_copy.wait()
    row_sum_copy.wait()
    quad_copy.wait()
    mix_copy.wait()
    row = lax.broadcasted_iota(jnp.int32, (everything, live_total), 0)
    lane = lax.broadcasted_iota(jnp.int32, (everything, live_total), 1)
    pick[...] = jnp.zeros_like(pick)

    def mark(i, begin):
        within = row - i * slots
        hit = (within >= 0) & (within < counts[i]) & (lane == begin + within)
        pick[...] += jnp.where(hit, 1.0, 0.0).astype(F32)
        return begin + counts[i]

    lax.fori_loop(0, n, mark, jnp.int32(0))
    quad_slot[...] = jnp.broadcast_to(
        jnp.sum(pick[...] * quad[...], axis=1, keepdims=True), quad_slot.shape
    )
    degree = lax.broadcasted_iota(jnp.int32, (degrees, channels), 0)
    lax.fori_loop(1, pairs, wait_moment, 0)
    totals = jnp.sum(sums[...], axis=0)
    mean = totals[0:1] / points
    variance = totals[1:2] / points - mean * mean
    gain[...] = gain[...] * lax.rsqrt(variance + 1e-05)
    def part(ref, piece, device):
        b, many, first, size = piece
        return ref.at[pl.ds(b, many), device, pl.ds(first, size)]

    def landing(p):
        if p < len(homeward) - 1:
            return part(back, homeward[p], me)
        return last.at[:, me]

    def return_copy(p, i):
        other = lax.rem(me + i, n)
        return pltpu.make_async_remote_copy(
            src_ref=part(outgoing, homeward[p], other), dst_ref=landing(p),
            send_sem=back_send.at[p, i], recv_sem=back_arrive.at[p, i],
            device_id={axis: other}, device_id_type=pl.DeviceIdType.MESH,
        )

    def return_own(p):
        return pltpu.make_async_copy(
            part(outgoing, homeward[p], me), landing(p), back_own.at[p]
        )

    for b in range(blocks):
        count = min(BLOCK, share - b * BLOCK)
        if count < BLOCK:
            result[...] = jnp.zeros_like(result)

        def wait_block(i, carry):
            block_copy(b, i).wait()
            return carry

        lax.fori_loop(1, n, wait_block, 0)
        own_copy(b).wait()

        def widen(i, carry):
            for s in range(slots):
                wide = recv[b, i, s].astype(F32)
                begin = pl.multiple_of((i * slots + s) * 2 * BLOCK, 8)
                for h in range(halves):
                    gathered[h, pl.ds(begin, 2 * BLOCK), :] = wide[:, h * 128 : (h + 1) * 128]
            return carry

        lax.fori_loop(0, n, widen, 0)

        def wave_step(r, carry):
            wave = owner[me * share + b * BLOCK + r]
            expanded = jnp.dot(
                pick[...].astype(BF16), legendre[b * BLOCK + r], preferred_element_type=F32
            ).astype(BF16)
            flag = jnp.where(wave == 0, 1.0, 0.0).astype(F32)
            parts = []
            for t in range(2):
                for h in range(halves):
                    lanes = slice(h * 128, (h + 1) * 128)
                    piece = gathered[h, pl.ds(t * BLOCK + r, everything, stride=2 * BLOCK), :]
                    if t == 0:
                        rest = gathered[h, pl.ds(BLOCK + r, everything, stride=2 * BLOCK), :]
                        piece = piece + rest * flag
                    else:
                        piece = piece * (1.0 - flag)
                    piece = piece - mean[:, lanes] * row_sum[t * waves + wave]
                    parts.append((piece * quad_slot[...]).astype(BF16))
            weighted = jnp.concatenate(parts, axis=1)
            coefficient = lax.dot_general(
                expanded, weighted, (((0,), (0,)), ((), ())), preferred_element_type=F32
            )
            kept = degree >= wave
            factor = jnp.where(wave > 0, 2.0, 1.0).astype(F32)
            mixed = []
            for t in range(2):
                part = coefficient[:, t * channels : (t + 1) * channels] * gain[...]
                part = jnp.where(kept, part, 0.0).astype(BF16)
                mixed.append(jnp.dot(part, mix[...], preferred_element_type=F32).astype(BF16))
            synthesis = jnp.dot(
                expanded, jnp.concatenate(mixed, axis=1), preferred_element_type=F32
            ) * factor
            for t in range(2):
                for h in range(halves):
                    begin = t * channels + h * 128
                    result[h, pl.ds(t * BLOCK + r, everything, stride=2 * BLOCK), :] = synthesis[
                        :, begin : begin + 128
                    ]
            return carry

        lax.fori_loop(0, count, wave_step, 0)

        def narrow(i, carry):
            for s in range(slots):
                begin = pl.multiple_of((i * slots + s) * 2 * BLOCK, 8)
                outgoing[b, i, s] = jnp.concatenate(
                    [result[h, pl.ds(begin, 2 * BLOCK), :] for h in range(halves)], axis=1
                ).astype(BF16)
            return carry

        lax.fori_loop(0, n, narrow, 0)

        for p, piece in enumerate(homeward):
            if piece[0] + piece[1] - 1 == b:

                def start_return(i, carry):
                    return_copy(p, i).start()
                    return carry

                lax.fori_loop(1, n, start_return, 0)
                return_own(p).start()

    def settle(p):
        def wait_return(i, carry):
            return_copy(p, i).wait()
            return carry

        lax.fori_loop(1, n, wait_return, 0)
        return_own(p).wait()

    def whole_slot(s, carry):
        block = back[:, :, s].reshape(blocks * lines, channels)
        partial[s] = jnp.dot(front[...], block, preferred_element_type=F32).astype(BF16)
        return carry

    def front_slot(s, carry):
        if held_back > 0:
            block = back[:held_back, :, s].reshape(split, channels)
            total = jnp.dot(front[:, :split], block, preferred_element_type=F32)
            partial[s] = total.astype(BF16)
        else:
            partial[s] = jnp.zeros(partial.shape[1:], BF16)
        return carry

    for p in range(held_back):
        settle(p)
    lax.fori_loop(ready, slots, front_slot, 0)
    for p in range(held_back, len(homeward) - 1):
        settle(p)
        lax.fori_loop(0, ready, whole_slot, 0)
    settle(len(homeward) - 1)


def inverse_kernel(last, table, partial, out, held, store):
    slots = partial.shape[0]
    ready = slots - last.shape[2]

    def store_slot(s):
        source = partial.at[s] if s < ready else held.at[s - ready]
        return pltpu.make_async_copy(source, out.at[s], store.at[s])

    for s in range(ready):
        store_slot(s).start()
    for s in range(ready, slots):
        block = last[:, :, s - ready].reshape(table.shape[1], last.shape[-1])
        total = jnp.dot(table[...], block, preferred_element_type=F32)
        held[s - ready] = (partial[s].astype(F32) + total).astype(BF16)
        store_slot(s).start()
    for s in range(slots):
        store_slot(s).wait()


def body(
    n, grid_values, lat_counts, owner_wavenumber, legendre, quad_weight, spectral_gain, channel_mix
):
    slots, longitudes, channels = grid_values.shape
    waves = owner_wavenumber.shape[0]
    share, live_total, degrees = legendre.shape
    blocks = -(-share // BLOCK)
    padded = blocks * BLOCK
    everything = n * slots
    trig = trig_table(waves, longitudes)
    base = jnp.asarray(trig)
    row_sum = jnp.asarray(trig.astype(np.float64).sum(axis=1).astype(np.float32))

    vmem = pl.BlockSpec(memory_space=pltpu.VMEM)
    anywhere = pl.BlockSpec(memory_space=pl.ANY)
    limit = 48 * 1024 * 1024
    far = functools.partial(pltpu.with_memory_space_constraint, memory_space=pltpu.HBM)
    packet = (blocks, n, slots, 2 * BLOCK, channels)
    copies = pltpu.SemaphoreType.DMA
    lines = n * 2 * BLOCK
    tail = min(TAIL, slots)
    late = max(blocks - HELD, 1)
    returns = len(homeward_pieces(blocks, slots, slots - tail, blocks - late))
    last, back_table, partial = pl.pallas_call(
        functools.partial(spectral_kernel, "lat", n, live_total * longitudes, share),
        out_shape=(
            pltpu.VMEM((late, n, tail) + packet[3:], BF16),
            pltpu.VMEM((longitudes, late * lines), BF16),
            pltpu.VMEM((slots, longitudes, channels), BF16),
        ),
        in_specs=[anywhere] * 9,
        out_specs=(vmem, vmem, vmem),
        scratch_shapes=[
            pltpu.SMEM(lat_counts.shape, jnp.int32),
            pltpu.SMEM(owner_wavenumber.shape, jnp.int32),
            pltpu.SMEM(row_sum.shape, F32),
            pltpu.VMEM((1, live_total), F32),
            pltpu.VMEM(channel_mix.shape, BF16),
            pltpu.VMEM((2, 2, channels), F32),
            pltpu.VMEM((n // 2, 2, channels), F32),
            pltpu.VMEM((n * padded, channels), F32),
            pltpu.VMEM((n * padded, waves), F32),
            pltpu.VMEM((blocks * lines, longitudes), BF16),
            pltpu.VMEM((longitudes, blocks * lines), BF16),
            pltpu.VMEM(packet, BF16),
            pltpu.VMEM(packet, BF16),
            pltpu.VMEM((channels // 128, everything * 2 * BLOCK, 128), F32),
            pltpu.VMEM((everything, live_total), F32),
            pltpu.VMEM((everything, 128), F32),
            pltpu.VMEM(packet, BF16),
            pltpu.VMEM((channels // 128, everything * 2 * BLOCK, 128), F32),
            pltpu.VMEM(packet, BF16),
            pltpu.VMEM(base.shape, BF16),
            pltpu.VMEM(legendre.shape, BF16),
            pltpu.VMEM(spectral_gain.shape, F32),
            copies((slots,)), copies((8,)),
            copies((n // 2,)), copies((n // 2,)),
            copies((blocks, n)), copies((blocks, n)), copies((blocks,)),
            copies((returns, n)), copies((returns, n)), copies((returns,)),
        ],
        compiler_params=pltpu.CompilerParams(
            collective_id=0, has_side_effects=True, vmem_limit_bytes=limit
        ),
    )(
        *map(far, (
            lat_counts, owner_wavenumber, row_sum, grid_values, base, legendre,
            quad_weight.reshape(1, live_total), spectral_gain, channel_mix,
        ))
    )

    return pl.pallas_call(
        inverse_kernel,
        out_shape=jax.ShapeDtypeStruct((slots, longitudes, channels), BF16),
        in_specs=[vmem, vmem, vmem],
        out_specs=anywhere,
        scratch_shapes=[
            pltpu.VMEM((tail, longitudes, channels), BF16),
            copies((slots,)),
        ],
        compiler_params=pltpu.CompilerParams(vmem_limit_bytes=16 * 1024 * 1024),
    )(*[pltpu.with_memory_space_constraint(v, pltpu.VMEM) for v in (last, back_table, partial)])


def solution(mesh):
    return jax.shard_map(
        functools.partial(body, mesh.shape["lat"]),
        mesh=mesh,
        in_specs=(P(("group", "lat"), None, None), P(), P(), P("lat", None, None), P(), P(), P()),
        out_specs=P(("group", "lat"), None, None),
        check_vma=False,
    )
```
